128 devices in a mesh: seq: 8 (over y_lo, x), exp: 16 (over y_hi, z, core).
Axes of the slice: x: 4, y: 4 (y_hi: 2, y_lo: 2; y = y_hi * 2 + y_lo), z: 4, core: 2. Of those that a mesh axis runs over, the one named last changes fastest.
Arguments:
- gates: float32 [16384, 2], P(('seq', 'exp')), may hold values from 0.1 to 0.9
- expert_ids: int32 [16384, 2], P(('seq', 'exp')), may hold values from 0 to 15, all different within a row; in each aligned block of 128 rows (0 to 127, 128 to 255, ...) at most 16 rows name the same one
- saved_pre: bfloat16 [16, 2048, 2, 7168], P('exp', None, None, 'seq'), may hold values from -6 to 6
- w_down: bfloat16 [16, 7168, 4096], P('exp', 'seq'), may hold values from -0.0625 to 0.0625
- residual_grad: bfloat16 [16384, 4096], P(('seq', 'exp')), may hold values from -6 to 6
- in_weight: bfloat16 [4096, 4096], P('seq', 'exp'), may hold values from -0.09375 to 0.09375
- ssm_in: bfloat16 [16384, 4096], P('seq', 'exp'), may hold values from -0.59765625 to 0.59765625
- b_proj: bfloat16 [16384, 128], P('seq'), may hold values from -0.546875 to 0.546875
- c_proj: bfloat16 [16384, 128], P('seq'), may hold values from -0.546875 to 0.546875
- step_sizes: float32 [64, 16384], P('exp', 'seq'), may hold values from 0.05 to 4590.52
- a_log: float32 [64], P('exp'), may hold values from -12 to 0
- skip_gain: float32 [64], P('exp'), may hold values from 0.5 to 1.5
- ssm_grad: bfloat16 [16384, 4096], P('seq', 'exp'), may hold values from -6 to 6
Outputs:
- pre_grads: bfloat16 [16, 2048, 2, 7168], P('exp', None, None, 'seq')
- route_grads: float32 [16384, 2], P(('seq', 'exp'))
- b_grads: float32 [16384, 128], P(('seq', 'exp'))
- c_grads: float32 [16384, 128], P(('seq', 'exp'))
- step_grads: float32 [64, 16384], P('exp', 'seq')
The draws below stay inside these ranges and needn't reach their ends.
Inputs may be any that keep to these rules, and one draw needn't show every extreme that they name: `expert_ids`: in each aligned block of 128 rows every expert is named by exactly 16 entries, and a row names 2 different experts.
All inputs are finite; a program needn't handle non-finite values.
Results may differ from the reference program's by a relative error of at most 0.019.
Values may be sent and summed in bfloat16 or wider, within the bound.
No kernel may reach another device: no remote copies, remote signals or barrier semaphores. Data moves between devices by JAX's collectives and lax.ppermute only.
A program may use at most 192 MiB of HBM per device.

```python
import math
import jax
import jax.numpy as jnp
import numpy as np
from jax import lax

D = 4096
FFW = 7168
EXPERTS = 16
TOPK = 2
TOK_DEV = 128
TIME_HORIZON = 16384
TOKENS = 16384
CAP = 16
ESLOTS = 2048
HEAD_DEV = 4
CHANNEL_GROUPS = 64
HDIM = 64
NSTATE = 128
SPAN = 256
N_SEQ = 8
N_EXP = 16


def rate_fields(key):
    sampler_seeds = jax.random.split(jax.random.fold_in(key, 11), 6)
    fast_share = 0.5
    fast_heads = jax.random.uniform(sampler_seeds[0], (CHANNEL_GROUPS,)) < fast_share
    fast_rate = jax.random.uniform(sampler_seeds[1], (CHANNEL_GROUPS,), minval=0.2, maxval=0.35)
    slow_rate = jnp.exp(jax.random.uniform(sampler_seeds[2], (CHANNEL_GROUPS,), minval=jnp.log(0.2), maxval=jnp.log(0.6))) / (0.11 * TIME_HORIZON)
    forgetting_multiplier = jnp.where(fast_heads, fast_rate, slow_rate)
    drawn_increments = jnp.exp(jax.random.uniform(sampler_seeds[3], (CHANNEL_GROUPS, TIME_HORIZON), minval=jnp.log(0.05), maxval=jnp.log(0.2)))
    surge_instant = jax.random.randint(sampler_seeds[4], (3,), 0, TIME_HORIZON)
    surge_indicator = jnp.any(jnp.arange(TIME_HORIZON)[None, :] == surge_instant[:, None], axis=0)
    surge_magnitude = jax.random.uniform(sampler_seeds[5], (CHANNEL_GROUPS, TIME_HORIZON), minval=0.22, maxval=0.5)
    increment_elements = jnp.where(surge_indicator[None, :], surge_magnitude / forgetting_multiplier[:, None], drawn_increments)
    return (jnp.log(forgetting_multiplier).astype(jnp.float32), increment_elements.astype(jnp.float32))


def draw_a_log(key, part):
    return rate_fields(key)[0]


def draw_step_sizes(key, part):
    return rate_fields(key)[1]


def block_scale(rng, shape, shards, smallest, top_value):
    gain, own = 1.0, jax.random.fold_in(rng, 6)
    for axis_at, shards_of in shards:
        draws = jnp.exp(jax.random.uniform(jax.random.fold_in(own, axis_at), (shards_of,), jnp.float32, smallest / len(shards), top_value / len(shards)))
        gain = gain * jnp.repeat(draws, shape[axis_at] // shards_of).reshape([-1 if axis == axis_at else 1 for axis in range(len(shape))])
    return gain


def deal_out(key, own, number, rows, count, top, bound, skew):
    order = jax.random.permutation(key, count)
    heavy_load, common = shares(count, rows * top, bound, skew, True), shares(count, rows * top, bound, skew, False)
    places = jnp.arange(count)

    def named(tallies, rotation):
        used = int((tallies > 0).sum())
        fixed = max(1, used // 4)
        shifted = fixed + (places - fixed + rotation * (used - fixed)) % max(1, count - fixed)
        return jnp.zeros((count,), jnp.int32).at[order[jnp.where(places < fixed, places, shifted)]].set(jnp.asarray(tallies, jnp.int32))

    tallies = jnp.where(number % 4 == 0, named(heavy_load, number // 4), named(common, number - number // 4 - 1))
    mixed = jax.random.permutation(jax.random.fold_in(own, 3), count)
    source_of, sink = mixed[0:count // 2 * 2:2], mixed[1:count // 2 * 2:2]
    room = jnp.minimum(tallies[source_of] - 1, bound - tallies[sink]) // 2
    room = jnp.where((source_of == order[0]) | (sink == order[0]) | (tallies[sink] == 0), 0, jnp.maximum(room, 0))
    shifted = jax.random.randint(jax.random.fold_in(own, 4), (count // 2,), 0, 1 << 20) % (room + 1)
    tallies = tallies.at[source_of].add(-shifted).at[sink].add(shifted)
    items = jnp.searchsorted(jnp.cumsum(tallies), jnp.arange(rows * top), side="right").astype(jnp.int32)
    table = items.reshape(top, rows).T
    table = table[jax.random.permutation(jax.random.fold_in(own, 1), rows)]
    rotation = jax.random.randint(jax.random.fold_in(own, 2), (rows, 1), 0, top)
    return jnp.take_along_axis(table, (jnp.arange(top)[None, :] + rotation) % top, axis=1)


def shares(number_of, total, bound, lean, full):
    weights = [(1 << 20) // math.isqrt(standing ** lean) + 1 for standing in range(1, number_of + 1)]
    largest = bound if full else min(bound, max(-(-total // number_of), total * weights[0] // sum(weights)))
    least = 1 if total - largest >= number_of - 1 else 0
    counts, spare = [largest] + [least] * (number_of - 1), total - largest - least * (number_of - 1)
    while spare > 0:
        free = [i for i in range(1, number_of) if counts[i] < largest] or [i for i in range(1, number_of) if counts[i] < bound]
        whole, remaining = sum([weights[i] for i in free]), spare
        for i in free:
            addition = min(bound - counts[i], max(1, remaining * weights[i] // whole), spare)
            counts[i] = counts[i] + addition
            spare = spare - addition
    return np.array(counts)


def gaussian(stream_key, shape, scale, reach, cuts=(), kind=jnp.bfloat16):
    values = scale * jax.random.normal(stream_key, shape, jnp.float32)
    if cuts:
        values = values * block_scale(stream_key, shape, cuts, -0.22, 0.18)
    return jnp.clip(values, -reach, reach).astype(kind)


def setup_inputs(seed: int = 0) -> dict:
    seeds = jax.random.split(jax.random.key(seed), 14)
    gates = jnp.clip(0.1 + 0.79999997 * jax.random.uniform(seeds[0], (TOKENS, TOPK), jnp.float32) ** block_scale(seeds[0], (TOKENS, TOPK), ((0, 128),), -0.2, 0.2), 0.1, 0.9)
    expert_ids_keys = jax.random.split(jax.random.fold_in(seeds[1], 1), TOKENS // TOK_DEV)
    expert_ids_turns = jax.random.permutation(jax.random.fold_in(seeds[1], 3), TOKENS // TOK_DEV)
    expert_ids = jax.vmap(lambda own, number: deal_out(jax.random.fold_in(seeds[1], 2), own, number, TOK_DEV, EXPERTS, TOPK, CAP, 0))(expert_ids_keys, expert_ids_turns).reshape((TOKENS, TOPK))
    saved_pre = gaussian(seeds[2], (EXPERTS, ESLOTS, 2, FFW), 1.0, 6.0, ((0, 16), (3, 8)))
    w_down = gaussian(seeds[3], (EXPERTS, FFW, D), FFW ** -0.5, 0.0625, ((0, 16), (1, 8)))
    residual_grad = gaussian(seeds[4], (TOKENS, D), 1.0, 6.0, ((0, 128),))
    in_weight = gaussian(seeds[5], (D, CHANNEL_GROUPS * HDIM), (CHANNEL_GROUPS * HDIM) ** -0.5, 0.09375, ((0, 8), (1, 16)))
    ssm_in = gaussian(seeds[6], (TIME_HORIZON, CHANNEL_GROUPS * HDIM), 0.1, 0.59765625, ((0, 8), (1, 16)))
    b_proj = gaussian(seeds[7], (TIME_HORIZON, NSTATE), 0.088, 0.546875, ((0, 8),))
    c_proj = gaussian(seeds[8], (TIME_HORIZON, NSTATE), 0.088, 0.546875, ((0, 8),))
    step_sizes = draw_step_sizes(jax.random.fold_in(seeds[13], 71), 0)
    a_log = draw_a_log(jax.random.fold_in(seeds[13], 71), 0)
    skip_gain = jnp.clip(0.5 + 1.0 * jax.random.uniform(seeds[11], (CHANNEL_GROUPS,), jnp.float32) ** block_scale(seeds[11], (CHANNEL_GROUPS,), ((0, 16),), -0.2, 0.2), 0.5, 1.5)
    ssm_grad = gaussian(seeds[12], (TIME_HORIZON, CHANNEL_GROUPS * HDIM), 1.0, 6.0, ((0, 8), (1, 16)))
    return dict(gates=gates, expert_ids=expert_ids, saved_pre=saved_pre, w_down=w_down, residual_grad=residual_grad, in_weight=in_weight, ssm_in=ssm_in, b_proj=b_proj, c_proj=c_proj, step_sizes=step_sizes, a_log=a_log, skip_gain=skip_gain, ssm_grad=ssm_grad)


PRECISE = lax.Precision.HIGHEST

def span_scan(heads_input, b_values, c_values, log_decay, skip_values, start_state):
    head_count, length, head_size = heads_input.shape
    state_size = b_values.shape[1]
    blocks = length // SPAN
    x_spans = heads_input.reshape(head_count, blocks, SPAN, head_size).transpose(1, 0, 2, 3)
    b_spans = b_values.reshape(blocks, SPAN, state_size)
    c_spans = c_values.reshape(blocks, SPAN, state_size)
    g_spans = log_decay.reshape(head_count, blocks, SPAN).transpose(1, 0, 2)
    lower_mask = jnp.tril(jnp.ones((SPAN, SPAN), jnp.bool_))

    def advance(carried_state, inputs):
        x_block, b_block, c_block, g_block = inputs
        cumulative = jnp.cumsum(g_block, axis=1)
        spread = cumulative[:, :, None] - cumulative[:, None, :]
        weights = jnp.where(lower_mask, jnp.exp(-jnp.where(lower_mask, spread, 0.0)), 0.0)
        scores = jnp.dot(c_block, b_block.T, precision=PRECISE)
        within = jnp.einsum('hij,ij,hjp->hip', weights, scores, x_block, precision=PRECISE)
        carried = jnp.einsum('hi,in,hpn->hip', jnp.exp(-cumulative), c_block, carried_state, precision=PRECISE)
        tail_decay = jnp.exp(cumulative - cumulative[:, -1:])
        fresh_state = jnp.einsum('hj,hjp,jn->hpn', tail_decay, x_block, b_block, precision=PRECISE)
        next_state = jnp.exp(-cumulative[:, -1])[:, None, None] * carried_state + fresh_state
        return (next_state, within + carried)
    final_state, outputs = lax.scan(advance, start_state, (x_spans, b_spans, c_spans, g_spans))
    output = outputs.transpose(1, 0, 2, 3).reshape(head_count, length, head_size)
    return (output + skip_values[:, None, None] * heads_input, final_state)

def swiglu_grads(upstream, gate_values, saved_rows):
    gate_pre = saved_rows[:, 0, :].astype(jnp.float32)
    up_pre = saved_rows[:, 1, :].astype(jnp.float32)
    sigmoid_gate = jax.nn.sigmoid(gate_pre)
    activated = gate_pre * sigmoid_gate
    route_part = lax.optimization_barrier(jnp.sum(activated * up_pre * upstream, axis=1))
    hidden_grad = gate_values[:, None] * upstream
    gate_grad = hidden_grad * up_pre * sigmoid_gate * (1.0 + gate_pre * (1.0 - sigmoid_gate))
    up_grad = hidden_grad * activated
    return (jnp.stack([gate_grad, up_grad], axis=1).astype(jnp.bfloat16), route_part)

def reference(gates, expert_ids, saved_pre, w_down, residual_grad, in_weight, ssm_in, b_proj, c_proj, step_sizes, a_log, skip_gain, ssm_grad):
    heads_input = ssm_in.astype(jnp.float32).reshape(TIME_HORIZON, CHANNEL_GROUPS, HDIM).transpose(1, 0, 2)
    grads_heads = ssm_grad.astype(jnp.float32).reshape(TIME_HORIZON, CHANNEL_GROUPS, HDIM).transpose(1, 0, 2)
    decay_rates = jnp.exp(a_log)

    def forward(inputs, b_values, c_values, sizes):
        outputs, unused = span_scan(inputs, b_values, c_values, sizes * decay_rates[:, None], skip_gain, jnp.zeros((CHANNEL_GROUPS, HDIM, NSTATE), jnp.float32))
        return outputs
    unused, pullback = jax.vjp(forward, heads_input, b_proj.astype(jnp.float32), c_proj.astype(jnp.float32), step_sizes)
    input_heads, b_grads, c_grads, step_grads = pullback(grads_heads)
    x_grad = input_heads.transpose(1, 0, 2).reshape(TIME_HORIZON, CHANNEL_GROUPS * HDIM).astype(jnp.bfloat16)
    group_width = HEAD_DEV * HDIM
    grad_groups = x_grad.reshape(TIME_HORIZON, N_EXP, group_width).transpose(1, 0, 2)
    weight_groups = in_weight.reshape(D, N_EXP, group_width).transpose(1, 0, 2)

    def add_group(total, pair):
        head_part = jnp.dot(pair[0], pair[1].T, preferred_element_type=jnp.float32).astype(jnp.bfloat16)
        head_part = lax.optimization_barrier(head_part).astype(jnp.float32)
        return (total + head_part, None)
    summed, unused_out = lax.scan(add_group, residual_grad.astype(jnp.float32), (grad_groups, weight_groups))
    moe_grad = summed.astype(jnp.bfloat16)
    device_count = N_SEQ * N_EXP
    per_block = expert_ids.reshape(device_count, TOK_DEV * TOPK)
    onehot = (per_block[:, :, None] == jnp.arange(EXPERTS, dtype=jnp.int32)[None, None, :]).astype(jnp.int32)
    running = jnp.cumsum(onehot, axis=1)
    position = lax.optimization_barrier(jnp.sum(onehot * running, axis=2)) - 1
    slot_row = (jnp.arange(device_count, dtype=jnp.int32)[:, None] * CAP + position).reshape(-1).astype(jnp.int32)
    expert_flat = per_block.reshape(-1).astype(jnp.int32)
    assignment = jnp.arange(TOKENS * TOPK, dtype=jnp.int32)
    table = jnp.zeros((EXPERTS, ESLOTS), jnp.int32).at[expert_flat, slot_row].set(assignment)
    gate_flat = gates.reshape(-1)

    def one_expert(expert_index):
        members = table[expert_index]
        row_block = moe_grad[members // TOPK]
        upstream = jnp.dot(row_block, w_down[expert_index].T, preferred_element_type=jnp.float32)
        return swiglu_grads(upstream, gate_flat[members], saved_pre[expert_index])
    pre_grads, route_slots = lax.map(one_expert, jnp.arange(EXPERTS, dtype=jnp.int32))
    route_grads = route_slots[expert_flat, slot_row].reshape(TOKENS, TOPK)
    return (pre_grads, route_grads, b_grads, c_grads, step_grads)
```

```python
import functools
import jax
import jax.numpy as jnp
from jax import lax
from jax.experimental import pallas as pl
from jax.experimental.pallas import tpu as pltpu
from jax.sharding import Mesh
from jax.sharding import PartitionSpec as P

F32 = jnp.float32
BF = jnp.bfloat16
HEADS, HDIM, NST, L = 4, 64, 128, 128
HP = HEADS * HDIM
NT = (((1,), (1,)), ((), ()))
TN = (((0,), (0,)), ((), ()))


def dot(a, b, dims=(((1,), (0,)), ((), ())), precision=None):
    return lax.dot_general(a, b, dims, precision=precision, preferred_element_type=F32)


def over_heads(cols):
    low = lax.broadcasted_iota(jnp.int32, (cols.shape[0], 128), 1) < HDIM
    return jnp.concatenate(
        [jnp.where(low, cols[:, h : h + 1], cols[:, h + 1 : h + 2]) for h in (0, 2)], axis=1
    )


def head_rows(rows):
    return jnp.concatenate(
        [jnp.broadcast_to(rows[h : h + 1, :], (HDIM, NST)) for h in range(HEADS)], axis=0
    )


def states_kernel(
    x_ref, g_ref, b_ref, c_ref, step_ref, alog_ref,
    cumr_ref, cumc_ref, sl_ref, gl_ref, dpre_ref, dpost_ref, pack_ref, q_ref,
):
    spans = sl_ref.shape[0]
    q_ref[...] = jnp.zeros_like(q_ref)
    q = step_ref[...] * jnp.exp(alog_ref[...])
    for c in range(spans):
        q_ref[8 * c : 8 * c + HEADS, :] = q[:, L * c : L * (c + 1)]
    row = lax.broadcasted_iota(jnp.int32, (L, L), 0)
    col = lax.broadcasted_iota(jnp.int32, (L, L), 1)
    upper = (row <= col).astype(F32)
    cum = dot(q_ref[...], upper, precision=lax.Precision.HIGHEST)
    cumr_ref[...] = cum.reshape(spans, 8, L)
    turned = cum.T
    for c in range(spans):
        cumc_ref[c] = turned[:, 8 * c : 8 * c + 8]

    def forward(c, carry):
        state, run = carry
        sl_ref[c] = state.astype(BF)
        dpre_ref[c] = jnp.exp(-run)
        at = pl.ds(pl.multiple_of(c * L, L), L)
        cols = cumc_ref[c]
        last = jnp.broadcast_to(cumr_ref[c][:, L - 1 : L], (8, NST))
        tail = jnp.exp(jnp.minimum(cols - cols[L - 1 : L, :], 0.0))
        decayed = (x_ref[at, :].astype(F32) * over_heads(tail)).astype(BF)
        fresh = dot(decayed, b_ref[at, :], TN)
        return (head_rows(jnp.exp(-last)) * state + fresh, run + last)

    zero = (jnp.zeros((HP, NST), F32), jnp.zeros((8, NST), F32))
    state, run = lax.fori_loop(0, spans, forward, zero)
    pack_ref[0:HP, :] = state.astype(BF)
    total = jnp.exp(-run)
    high = total.astype(BF).astype(F32)
    pack_ref[2 * HP : 2 * HP + 16, :] = jnp.concatenate([high, total - high], axis=0).astype(BF)

    def backward(i, carry):
        state, run = carry
        c = spans - 1 - i
        gl_ref[c] = state.astype(BF)
        dpost_ref[c] = jnp.exp(-run)
        at = pl.ds(pl.multiple_of(c * L, L), L)
        last = jnp.broadcast_to(cumr_ref[c][:, L - 1 : L], (8, NST))
        decayed = (g_ref[at, :].astype(F32) * over_heads(jnp.exp(-cumc_ref[c]))).astype(BF)
        fresh = dot(decayed, c_ref[at, :], TN)
        return (head_rows(jnp.exp(-last)) * state + fresh, run + last)

    state, run = lax.fori_loop(0, spans, backward, zero)
    pack_ref[HP : 2 * HP, :] = state.astype(BF)


def local_states(x, g, b, c, step, alog):
    spans = x.shape[0] // L
    out = (
        jax.ShapeDtypeStruct((spans, 8, L), F32),
        jax.ShapeDtypeStruct((spans, L, 8), F32),
        jax.ShapeDtypeStruct((spans, HP, NST), BF),
        jax.ShapeDtypeStruct((spans, HP, NST), BF),
        jax.ShapeDtypeStruct((spans, 8, NST), F32),
        jax.ShapeDtypeStruct((spans, 8, NST), F32),
        jax.ShapeDtypeStruct((2 * HP + 16, NST), BF),
    )
    return pl.pallas_call(
        states_kernel,
        out_shape=out,
        scratch_shapes=[pltpu.VMEM((8 * spans, L), F32)],
        name="states",
    )(x, g, b, c, step, alog)


def grads_kernel(
    me_ref, x_ref, g_ref, b_ref, c_ref, cumr_ref, cumc_ref, sl_ref, gl_ref, dpre_ref, dpost_ref,
    packs_ref, alog_ref, skip_ref,
    dx_ref, bc_ref, dq_ref, sin_ref, gex_ref,
):
    count = packs_ref.shape[0]

    @pl.when(pl.program_id(0) == 0)
    def _():
        me = me_ref[0]

        def dec(s):
            both = packs_ref[s, 2 * HP : 2 * HP + 16, :].astype(F32)
            return head_rows(both[0:8] + both[8:16])

        sin_ref[...] = jnp.zeros_like(sin_ref)
        gex_ref[...] = jnp.zeros_like(gex_ref)
        for s in range(count):
            @pl.when(s < me)
            def _():
                sin_ref[...] = dec(s) * sin_ref[...] + packs_ref[s, 0:HP, :].astype(F32)
        for s in reversed(range(count)):
            @pl.when(s > me)
            def _():
                gex_ref[...] = dec(s) * gex_ref[...] + packs_ref[s, HP : 2 * HP, :].astype(F32)

    x = x_ref[...]
    g = g_ref[...]
    b = b_ref[...]
    c = c_ref[...]
    xf = x.astype(F32)
    gf = g.astype(F32)
    rows = cumr_ref[0]
    cols = cumc_ref[0]
    state = sl_ref[0].astype(F32) + head_rows(dpre_ref[0]) * sin_ref[...]
    after = gl_ref[0].astype(F32) + head_rows(dpost_ref[0]) * gex_ref[...]
    state_b = state.astype(BF)
    after_b = after.astype(BF)
    into = over_heads(jnp.exp(-cols))
    tail = over_heads(jnp.exp(jnp.minimum(cols - cols[L - 1 : L, :], 0.0)))
    g_in = (gf * into).astype(BF)
    x_tail = (xf * tail).astype(BF)
    dc = dot(g_in, state_b)
    db = dot(x_tail, after_b)
    from_after = dot(b, after_b, NT) * tail
    carried = dot(c, state_b, NT) * into
    scores = dot(c, b, NT)
    row = lax.broadcasted_iota(jnp.int32, (L, L), 0)
    col = lax.broadcasted_iota(jnp.int32, (L, L), 1)
    lower = row >= col
    before = (row < col).astype(BF)
    lower_b = lower.astype(BF)
    picks = (
        lax.broadcasted_iota(jnp.int32, (8, HP), 1) // HDIM
        == lax.broadcasted_iota(jnp.int32, (8, HP), 0)
    ).astype(BF)
    late = dot(picks, (gf * carried).astype(BF), NT)
    early = dot(picks, (xf * from_after).astype(BF), NT)
    across = jnp.sum(dot(picks, (state * after).astype(BF)), axis=1, keepdims=True)
    steps = (
        dot(late.astype(BF), lower_b)
        + dot(early.astype(BF), before)
        + across * jnp.exp(-rows[:, L - 1 : L])
    )
    mixed = jnp.zeros((L, L), F32)
    inner = []
    pieces = []
    for h in range(HEADS):
        at = slice(HDIM * h, HDIM * (h + 1))
        g_h = g[:, at]
        cross = dot(g_h, x[:, at], NT)
        decay = jnp.where(
            lower, jnp.exp(jnp.minimum(rows[h : h + 1, :] - cols[:, h : h + 1], 0.0)), 0.0
        )
        kept = decay * cross
        mixed = mixed + kept
        pieces.append(dot((decay * scores).astype(BF), g_h, TN))
        passed = dot((kept * scores).astype(BF), before)
        inner.append(jnp.sum(jnp.where(lower, passed, 0.0), axis=0, keepdims=True))
    steps = steps[0:HEADS] + jnp.concatenate(inner, axis=0)
    dq_ref[...] = -steps * jnp.exp(alog_ref[...])
    dx = jnp.concatenate(pieces, axis=1) + from_after + gf * skip_ref[...]
    dx_b = dx.astype(dx_ref.dtype)
    for q in range(dx_ref.shape[0]):
        dx_ref[q, 0, 0] = dx_b
    mixed_b = mixed.astype(BF)
    bc_ref[:, 0:NST] = (db + dot(mixed_b, c, TN)).astype(bc_ref.dtype)
    bc_ref[:, NST:] = (dc + dot(mixed_b, b)).astype(bc_ref.dtype)


def span_grads(me, x, g, b, c, parts, packs, alog, skip, half):
    cumr, cumc, sl, gl, dpre, dpost = parts
    spans = sl.shape[0] // 2
    base = half * spans
    once = lambda shape: pl.BlockSpec(shape, lambda i: (0,) * len(shape))
    lead = lambda shape: pl.BlockSpec((1, *shape), lambda i: (base + i, 0, 0))
    rows = lambda width: pl.BlockSpec((L, width), lambda i: (base + i, 0))
    return pl.pallas_call(
        grads_kernel,
        grid=(spans,),
        in_specs=[
            pl.BlockSpec(memory_space=pltpu.SMEM),
            rows(HP), rows(HP), rows(NST), rows(NST),
            lead((8, L)), lead((L, 8)), lead((HP, NST)), lead((HP, NST)),
            lead((8, NST)), lead((8, NST)),
            once(packs.shape), once(alog.shape), once(skip.shape),
        ],
        out_specs=[
            pl.BlockSpec((4, 1, 1, L, HP), lambda i: (0, i % 4, i // 4, 0, 0)),
            pl.BlockSpec((L, 2 * NST), lambda i: (i, 0)),
            pl.BlockSpec((HEADS, L), lambda i: (0, i)),
        ],
        out_shape=(
            jax.ShapeDtypeStruct((4, 4, spans // 4, L, HP), BF),
            jax.ShapeDtypeStruct((spans * L, 2 * NST), BF),
            jax.ShapeDtypeStruct((HEADS, spans * L), F32),
        ),
        scratch_shapes=[pltpu.VMEM((HP, NST), F32), pltpu.VMEM((HP, NST), F32)],
        cost_estimate=pl.CostEstimate(
            flops=4 << 30, bytes_accessed=8 << 20, transcendentals=spans * HEADS * L * L
        ),
        name="span_grads",
    )(me, x, g, b, c, cumr, cumc, sl, gl, dpre, dpost, packs, alog, skip)


def routing_kernel(ids_ref, gates_ref, tgt_ref, out_ref):
    experts, slots = out_ref.shape
    tokens = ids_ref.shape[1]
    expert = lax.broadcasted_iota(jnp.int32, (experts, tokens), 0)
    slot = lax.broadcasted_iota(jnp.int32, (slots, tokens), 0)
    named = [(expert == ids_ref[k : k + 1, :]).astype(F32) for k in range(2)]
    earlier = (
        lax.broadcasted_iota(jnp.int32, (tokens, tokens), 0)
        < lax.broadcasted_iota(jnp.int32, (tokens, tokens), 1)
    ).astype(BF)
    counts = dot((named[0] + named[1]).astype(BF), earlier)
    tgt_ref[...] = jnp.zeros_like(tgt_ref)
    total = jnp.zeros((experts, slots), F32)
    for k in range(2):
        position = jnp.sum(named[k] * counts, axis=0, keepdims=True).astype(jnp.int32)
        tgt_ref[k : k + 1, :] = ids_ref[k : k + 1, :] * slots + position
        placed = (slot == position).astype(BF)
        total = total + dot((named[k] * gates_ref[k : k + 1, :]).astype(BF), placed, NT)
    out_ref[...] = total.astype(out_ref.dtype)


def routing(ids, gates):
    return pl.pallas_call(
        routing_kernel,
        out_shape=(
            jax.ShapeDtypeStruct((8, ids.shape[1]), jnp.int32),
            jax.ShapeDtypeStruct((16, 16), BF),
        ),
        name="routing",
    )(ids, gates)


def rows_kernel(x_ref, w_ref, res_ref, tgt_ref, out_ref):
    left = jnp.concatenate([x_ref[e] for e in range(16)], axis=1)
    right = jnp.concatenate([w_ref[0, e % 4, e // 4] for e in range(16)], axis=1)
    total = dot(left, right, NT)
    slot = lax.broadcasted_iota(jnp.int32, (256, 128), 0)
    for k in range(2):
        rows = (res_ref[k].astype(F32) + total[128 * k : 128 * (k + 1)]).astype(BF)
        picks = (slot == tgt_ref[k, 0:1, :]) | (slot == tgt_ref[k, 1:2, :])
        out_ref[:, k] = dot(picks.astype(BF), rows).astype(BF).reshape(16, 16, 128)


def expert_rows(x, weight, residual, targets, half):
    return pl.pallas_call(
        rows_kernel,
        grid=(8,),
        in_specs=[
            pl.BlockSpec((16, 256, 256), lambda s: (0, 0, 0)),
            pl.BlockSpec((1, 4, 4, 128, 256), lambda s: (s, 0, 0, 0, 0)),
            pl.BlockSpec((2, 128, 128), lambda s: (half, 0, s)),
            pl.BlockSpec((2, 8, 128), lambda s: (half, 0, 0)),
        ],
        out_specs=pl.BlockSpec((16, 2, 16, 128), lambda s: (0, 0, 0, s)),
        out_shape=jax.ShapeDtypeStruct((16, 2, 16, 1024), BF),
        compiler_params=pltpu.CompilerParams(vmem_limit_bytes=48 << 20),
        name="expert_rows",
    )(x, weight, residual, targets)


def expert_kernel(half, at_ref, own, left, right, low, high, w_hbm, saved, gates, *rest):
    out, route_ref, xbuf, wbuf, sbuf, gbuf, obuf, up_ref, psum_ref, sems = rest[-10:]
    x_at, y_at = at_ref[0], at_ref[1]
    saved_copy = pltpu.make_async_copy(saved.at[y_at, :, half], sbuf, sems.at[4])
    gates_copy = pltpu.make_async_copy(gates.at[y_at, :, half], gbuf, sems.at[5])
    tiles = [(0, 256), (256, 512), (512, 768), (768, 896)]
    weights = [
        pltpu.make_async_copy(w_hbm.at[a:b, :], wbuf.at[a:b, :], sems.at[i])
        for i, (a, b) in enumerate(tiles)
    ]
    copies = []
    for piece, step, first in ((own, 0, 0), (left, 3, 0), (right, 1, 0), (low, 2, 0), (high, 2, 2)):
        source = lax.rem(x_at + step, 4)
        for q in range(piece.shape[0]):
            for k in range(2):
                lanes = slice(1024 * (first + q), 1024 * (first + q + 1))
                copies.append(
                    pltpu.make_async_copy(
                        piece.at[q, :, k], xbuf.at[source, k, :, :, lanes], sems.at[6 + len(copies)]
                    )
                )
    weights[0].start()
    for copy in copies:
        copy.start()
    for copy in weights[1:]:
        copy.start()
    gates_copy.start()
    saved_copy.start()
    for copy in copies:
        copy.wait()
    x = xbuf[...].reshape(512, 4096)
    for i, (a, b) in enumerate(tiles):
        weights[i].wait()
        turned = jnp.concatenate(
            [
                wbuf[a:b, 512 * s + 128 * q : 512 * s + 128 * (q + 1)]
                for q in range(4)
                for s in range(8)
            ],
            axis=1,
        )
        width = b - a
        up_ref[:, 0:width] = dot(x, turned, NT)
        if i == 0:
            gates_copy.wait()
            saved_copy.wait()
            psum_ref[...] = jnp.zeros_like(psum_ref)

        def group(j, carry):
            rows = pl.ds(pl.multiple_of(j * 128, 128), 128)
            upstream = up_ref[rows, 0:width]
            gate_pre = sbuf[j, :, 0, a:b].astype(F32)
            up_pre = sbuf[j, :, 1, a:b].astype(F32)
            sigmoid = 1.0 / (1.0 + jnp.exp(-gate_pre))
            active = gate_pre * sigmoid
            weighted = gbuf[j] * upstream
            part = active * up_pre * upstream
            gate_grad = weighted * up_pre * sigmoid * (1.0 + gate_pre * (1.0 - sigmoid))
            obuf[j, :, 0, a:b] = gate_grad.astype(BF)
            obuf[j, :, 1, a:b] = (weighted * active).astype(BF)
            both = part[:, 0:128]
            if width == 256:
                both = both + part[:, 128:256]
            psum_ref[rows, :] = psum_ref[rows, :] + both
            return carry

        lax.fori_loop(0, 4, group, 0)
    out_copy = pltpu.make_async_copy(obuf, out.at[y_at, :, half], sems.at[4])
    out_copy.start()
    ones = jnp.ones((8, 128), F32)
    route_ref[...] = dot(ones, psum_ref[...], NT, precision=lax.Precision.HIGHEST)
    out_copy.wait()


def expert_grads(half, at, pieces, weight, saved, gates, before):
    own, left, right, low, high = [p.reshape(-1, 4, 2, 16, 1024) for p in pieces]
    hbm = pl.BlockSpec(memory_space=pl.ANY)
    args = [at, own, left, right, low, high, weight, saved, gates]
    if before is not None:
        args.append(before)
    return pl.pallas_call(
        functools.partial(expert_kernel, half),
        in_specs=[pl.BlockSpec(memory_space=pltpu.SMEM)] + [hbm] * (len(args) - 1),
        out_specs=[hbm, pl.BlockSpec(memory_space=pltpu.VMEM)],
        out_shape=(
            jax.ShapeDtypeStruct(saved.shape, BF),
            jax.ShapeDtypeStruct((8, 512), F32),
        ),
        scratch_shapes=[
            pltpu.VMEM((4, 2, 4, 16, 4096), BF),
            pltpu.VMEM((896, 4096), BF),
            pltpu.VMEM((4, 128, 2, 896), BF),
            pltpu.VMEM((4, 128, 1), F32),
            pltpu.VMEM((4, 128, 2, 896), BF),
            pltpu.VMEM((512, 256), F32),
            pltpu.VMEM((512, 128), F32),
            pltpu.SemaphoreType.DMA((40,)),
        ],
        input_output_aliases={} if before is None else {9: 0},
        compiler_params=pltpu.CompilerParams(vmem_limit_bytes=56 << 20),
        cost_estimate=pl.CostEstimate(
            flops=2 * 512 * 896 * 4096, bytes_accessed=16 << 20, transcendentals=512 * 896
        ),
        name="expert_grads",
    )(*args)


SEQ = ("yl", "x")
QUAD = ("yh", "zh")
MEMB = ("zl", "core")
EXP = QUAD + MEMB
BOTH = SEQ + EXP


def a2a(array, axis):
    return lax.all_to_all(array, axis, split_axis=0, concat_axis=0, tiled=True)


def shifted(array, by):
    return lax.ppermute(array, "x", [(i, (i + by) % 4) for i in range(4)])


def other_row(array):
    return lax.ppermute(array, "yl", [(0, 1), (1, 0)])


def along_x(own):
    left = shifted(own, 1)
    right = shifted(own, -1)
    low = shifted(left[:8], 1)
    high = shifted(right[8:], -1)
    return (own, left, right, low, high)


def per_device(
    gates, expert_ids, saved_pre, w_down, residual_grad, in_weight,
    ssm_in, b_proj, c_proj, step_sizes, a_log, skip_gain, ssm_grad,
):
    quarters = a2a(in_weight.reshape(4, 128, 256), QUAD)
    weight = lax.all_gather(quarters.reshape(512, 256), SEQ + MEMB, axis=0, tiled=True)
    weight = weight.reshape(8, 4, 4, 128, 256)

    alog = a_log.reshape(4, 1)
    skip = jnp.repeat(skip_gain, HDIM).reshape(1, HP)
    *parts, pack = local_states(ssm_in, ssm_grad, b_proj, c_proj, step_sizes, alog)
    packs = a2a(jnp.broadcast_to(pack, (8, *pack.shape)), SEQ)

    targets, slot_gates = routing(expert_ids.T, gates.T)
    all_targets = lax.all_gather(targets, QUAD, axis=0)
    residual = residual_grad.reshape(128, 8, 4, 128).transpose(2, 0, 1, 3)
    residual = a2a(residual.reshape(4, 128, 1024), QUAD)

    here = lax.axis_index(SEQ).reshape(1)
    args = (here, ssm_in, ssm_grad, b_proj, c_proj, parts, packs, alog, skip)
    arrived, grads = {}, {}
    for half in (1, 0):
        x_part, bc_part, step_part = span_grads(*args, half)
        grads[half] = (bc_part, step_part)
        moved = a2a(x_part.reshape(16, 256, 256), EXP)
        rows = expert_rows(moved, weight, residual, all_targets, half)
        arrived[half] = a2a(rows.reshape(16, 32, 1024), EXP)

    gate_rows = lax.all_gather(a2a(slot_gates, EXP), SEQ, axis=0)
    gate_rows = gate_rows.astype(F32).reshape(2, 4, 2, 128, 1)

    mine = along_x(arrived[1])
    theirs = tuple(other_row(p) for p in mine)
    partner = other_row(arrived[0])
    sets = [(1, 0, mine), (0, 0, along_x(arrived[0])), (1, 1, theirs), (0, 1, along_x(partner))]

    x_at, y_at = lax.axis_index("x"), lax.axis_index("yl")
    saved = saved_pre.reshape(2, 4, 2, 128, 2, 896)
    out, routes = None, {}
    for half, flip, pieces in sets:
        at = jnp.stack([x_at, y_at ^ flip]).astype(jnp.int32)
        out, route = expert_grads(half, at, pieces, w_down[0], saved, gate_rows, out)
        routes[half, flip] = route[0].reshape(4, 128)
    first, second = [
        jnp.stack([routes[0, flip], routes[1, flip]], axis=1).reshape(4, 256) for flip in (0, 1)
    ]
    low, high = [jnp.where(y_at == 0, a, b) for a, b in ((first, second), (second, first))]
    partial = jnp.concatenate([low, high], axis=0)
    summed = jnp.sum(a2a(partial, SEQ), axis=0)
    totals = a2a(summed.reshape(16, 16), EXP).reshape(256, 1)
    slot = lax.broadcasted_iota(jnp.int32, (256, 128), 0)
    route_grads = jnp.stack(
        [jnp.sum(jnp.where(slot == targets[k], totals, 0.0), axis=0) for k in range(2)], axis=1
    )

    both = jnp.concatenate([grads[0][0], grads[1][0]], axis=0).reshape(16, 128, 2 * NST)
    both = jnp.sum(a2a(both, EXP).astype(F32), axis=0)
    step_grads = jnp.concatenate([grads[0][1], grads[1][1]], axis=1)
    pre_grads = out.reshape(1, 2048, 2, 896)
    return (pre_grads, route_grads, both[:, :NST], both[:, NST:], step_grads)


def solution(mesh):
    split = Mesh(mesh.devices.reshape(2, 4, 2, 2, 2, 2), BOTH)
    in_specs = (
        P(BOTH, None), P(BOTH, None), P(EXP, None, None, SEQ), P(EXP, SEQ, None), P(BOTH, None),
        P(SEQ, EXP), P(SEQ, EXP), P(SEQ, None), P(SEQ, None), P(EXP, SEQ), P(EXP), P(EXP),
        P(SEQ, EXP),
    )
    out_specs = (P(EXP, None, None, SEQ), P(BOTH, None), P(BOTH, None), P(BOTH, None), P(EXP, SEQ))
    return jax.shard_map(
        per_device, mesh=split, in_specs=in_specs, out_specs=out_specs, check_vma=False
    )
```

```python
import functools
import jax
import jax.numpy as jnp
from jax import lax
from jax.experimental import pallas as pl
from jax.experimental.pallas import tpu as pltpu
from jax.sharding import Mesh
from jax.sharding import PartitionSpec as P

F32 = jnp.float32
BF = jnp.bfloat16
HEADS, HDIM, NST, L = 4, 64, 128, 128
HP = HEADS * HDIM
NT = (((1,), (1,)), ((), ()))
TN = (((0,), (0,)), ((), ()))


def dot(a, b, dims=(((1,), (0,)), ((), ())), precision=None):
    return lax.dot_general(a, b, dims, precision=precision, preferred_element_type=F32)


def cost(us):
    return pl.CostEstimate(flops=int(us * 5e8), bytes_accessed=1 << 20, transcendentals=0)


def over_heads(cols):
    low = lax.broadcasted_iota(jnp.int32, (cols.shape[0], 128), 1) < HDIM
    return jnp.concatenate(
        [jnp.where(low, cols[:, h : h + 1], cols[:, h + 1 : h + 2]) for h in (0, 2)], axis=1
    )


def head_rows(rows):
    return jnp.concatenate(
        [jnp.broadcast_to(rows[h : h + 1, :], (HDIM, NST)) for h in range(HEADS)], axis=0
    )


def states_kernel(
    x_ref, g_ref, b_ref, c_ref, step_ref, alog_ref,
    cumr_ref, cumc_ref, sl_ref, gl_ref, dpre_ref, dpost_ref, pack_ref, q_ref,
):
    spans = sl_ref.shape[0]
    q_ref[...] = jnp.zeros_like(q_ref)
    q = step_ref[...] * jnp.exp(alog_ref[...])
    for c in range(spans):
        q_ref[8 * c : 8 * c + HEADS, :] = q[:, L * c : L * (c + 1)]
    row = lax.broadcasted_iota(jnp.int32, (L, L), 0)
    col = lax.broadcasted_iota(jnp.int32, (L, L), 1)
    upper = (row <= col).astype(F32)
    cum = dot(q_ref[...], upper, precision=lax.Precision.HIGHEST)
    cumr_ref[...] = cum.reshape(spans, 8, L)
    turned = cum.T
    for c in range(spans):
        cumc_ref[c] = turned[:, 8 * c : 8 * c + 8]

    def forward(c, carry):
        state, run = carry
        sl_ref[c] = state.astype(BF)
        dpre_ref[c] = jnp.exp(-run)
        at = pl.ds(pl.multiple_of(c * L, L), L)
        cols = cumc_ref[c]
        last = jnp.broadcast_to(cumr_ref[c][:, L - 1 : L], (8, NST))
        tail = jnp.exp(jnp.minimum(cols - cols[L - 1 : L, :], 0.0))
        decayed = (x_ref[at, :].astype(F32) * over_heads(tail)).astype(BF)
        fresh = dot(decayed, b_ref[at, :], TN)
        return (head_rows(jnp.exp(-last)) * state + fresh, run + last)

    zero = (jnp.zeros((HP, NST), F32), jnp.zeros((8, NST), F32))
    state, run = lax.fori_loop(0, spans, forward, zero)
    pack_ref[0:HP, :] = state.astype(BF)
    total = jnp.exp(-run)
    high = total.astype(BF).astype(F32)
    pack_ref[2 * HP : 2 * HP + 16, :] = jnp.concatenate([high, total - high], axis=0).astype(BF)

    def backward(i, carry):
        state, run = carry
        c = spans - 1 - i
        gl_ref[c] = state.astype(BF)
        dpost_ref[c] = jnp.exp(-run)
        at = pl.ds(pl.multiple_of(c * L, L), L)
        last = jnp.broadcast_to(cumr_ref[c][:, L - 1 : L], (8, NST))
        decayed = (g_ref[at, :].astype(F32) * over_heads(jnp.exp(-cumc_ref[c]))).astype(BF)
        fresh = dot(decayed, c_ref[at, :], TN)
        return (head_rows(jnp.exp(-last)) * state + fresh, run + last)

    state, run = lax.fori_loop(0, spans, backward, zero)
    pack_ref[HP : 2 * HP, :] = state.astype(BF)


def local_states(x, g, b, c, step, alog):
    spans = x.shape[0] // L
    out = (
        jax.ShapeDtypeStruct((spans, 8, L), F32),
        jax.ShapeDtypeStruct((spans, L, 8), F32),
        jax.ShapeDtypeStruct((spans, HP, NST), BF),
        jax.ShapeDtypeStruct((spans, HP, NST), BF),
        jax.ShapeDtypeStruct((spans, 8, NST), F32),
        jax.ShapeDtypeStruct((spans, 8, NST), F32),
        jax.ShapeDtypeStruct((2 * HP + 16, NST), BF),
    )
    return pl.pallas_call(
        states_kernel,
        out_shape=out,
        scratch_shapes=[pltpu.VMEM((8 * spans, L), F32)],
        cost_estimate=cost(16),
        name="states",
    )(x, g, b, c, step, alog)


def grads_kernel(
    me_ref, x_ref, g_ref, b_ref, c_ref, cumr_ref, cumc_ref, sl_ref, gl_ref, dpre_ref, dpost_ref,
    packs_ref, alog_ref, skip_ref,
    dx_ref, bc_ref, dq_ref, sin_ref, gex_ref,
):
    count = packs_ref.shape[0]

    @pl.when(pl.program_id(0) == 0)
    def _():
        me = me_ref[0]

        def dec(s):
            both = packs_ref[s, 2 * HP : 2 * HP + 16, :].astype(F32)
            return head_rows(both[0:8] + both[8:16])

        sin_ref[...] = jnp.zeros_like(sin_ref)
        gex_ref[...] = jnp.zeros_like(gex_ref)
        for s in range(count):
            @pl.when(s < me)
            def _():
                sin_ref[...] = dec(s) * sin_ref[...] + packs_ref[s, 0:HP, :].astype(F32)
        for s in reversed(range(count)):
            @pl.when(s > me)
            def _():
                gex_ref[...] = dec(s) * gex_ref[...] + packs_ref[s, HP : 2 * HP, :].astype(F32)

    x = x_ref[...]
    g = g_ref[...]
    b = b_ref[...]
    c = c_ref[...]
    xf = x.astype(F32)
    gf = g.astype(F32)
    rows = cumr_ref[0]
    cols = cumc_ref[0]
    state = sl_ref[0].astype(F32) + head_rows(dpre_ref[0]) * sin_ref[...]
    after = gl_ref[0].astype(F32) + head_rows(dpost_ref[0]) * gex_ref[...]
    state_b = state.astype(BF)
    after_b = after.astype(BF)
    into = over_heads(jnp.exp(-cols))
    tail = over_heads(jnp.exp(jnp.minimum(cols - cols[L - 1 : L, :], 0.0)))
    g_in = (gf * into).astype(BF)
    x_tail = (xf * tail).astype(BF)
    dc = dot(g_in, state_b)
    db = dot(x_tail, after_b)
    from_after = dot(b, after_b, NT) * tail
    carried = dot(c, state_b, NT) * into
    scores = dot(c, b, NT)
    row = lax.broadcasted_iota(jnp.int32, (L, L), 0)
    col = lax.broadcasted_iota(jnp.int32, (L, L), 1)
    lower = row >= col
    before = (row < col).astype(BF)
    lower_b = lower.astype(BF)
    picks = (
        lax.broadcasted_iota(jnp.int32, (8, HP), 1) // HDIM
        == lax.broadcasted_iota(jnp.int32, (8, HP), 0)
    ).astype(BF)
    late = dot(picks, (gf * carried).astype(BF), NT)
    early = dot(picks, (xf * from_after).astype(BF), NT)
    across = jnp.sum(dot(picks, (state * after).astype(BF)), axis=1, keepdims=True)
    steps = (
        dot(late.astype(BF), lower_b)
        + dot(early.astype(BF), before)
        + across * jnp.exp(-rows[:, L - 1 : L])
    )
    mixed = jnp.zeros((L, L), F32)
    inner = []
    pieces = []
    for h in range(HEADS):
        at = slice(HDIM * h, HDIM * (h + 1))
        g_h = g[:, at]
        cross = dot(g_h, x[:, at], NT)
        decay = jnp.where(
            lower, jnp.exp(jnp.minimum(rows[h : h + 1, :] - cols[:, h : h + 1], 0.0)), 0.0
        )
        kept = decay * cross
        mixed = mixed + kept
        pieces.append(dot((decay * scores).astype(BF), g_h, TN))
        passed = dot((kept * scores).astype(BF), before)
        inner.append(jnp.sum(jnp.where(lower, passed, 0.0), axis=0, keepdims=True))
    steps = steps[0:HEADS] + jnp.concatenate(inner, axis=0)
    dq_ref[...] = -steps * jnp.exp(alog_ref[...])
    dx = jnp.concatenate(pieces, axis=1) + from_after + gf * skip_ref[...]
    dx_b = dx.astype(dx_ref.dtype)
    for q in range(dx_ref.shape[0]):
        dx_ref[q, 0, 0] = dx_b
    mixed_b = mixed.astype(BF)
    bc_ref[:, 0:NST] = (db + dot(mixed_b, c, TN)).astype(bc_ref.dtype)
    bc_ref[:, NST:] = (dc + dot(mixed_b, b)).astype(bc_ref.dtype)


def span_grads(me, x, g, b, c, parts, packs, alog, skip, half):
    cumr, cumc, sl, gl, dpre, dpost = parts
    spans = sl.shape[0] // 2
    base = half * spans
    once = lambda shape: pl.BlockSpec(shape, lambda i: (0,) * len(shape))
    lead = lambda shape: pl.BlockSpec((1, *shape), lambda i: (base + i, 0, 0))
    rows = lambda width: pl.BlockSpec((L, width), lambda i: (base + i, 0))
    return pl.pallas_call(
        grads_kernel,
        grid=(spans,),
        in_specs=[
            pl.BlockSpec(memory_space=pltpu.SMEM),
            rows(HP), rows(HP), rows(NST), rows(NST),
            lead((8, L)), lead((L, 8)), lead((HP, NST)), lead((HP, NST)),
            lead((8, NST)), lead((8, NST)),
            once(packs.shape), once(alog.shape), once(skip.shape),
        ],
        out_specs=[
            pl.BlockSpec((4, 1, 1, L, HP), lambda i: (0, i % 4, i // 4, 0, 0)),
            pl.BlockSpec((L, 2 * NST), lambda i: (i, 0)),
            pl.BlockSpec((HEADS, L), lambda i: (0, i)),
        ],
        out_shape=(
            jax.ShapeDtypeStruct((4, 4, spans // 4, L, HP), BF),
            jax.ShapeDtypeStruct((spans * L, 2 * NST), BF),
            jax.ShapeDtypeStruct((HEADS, spans * L), F32),
        ),
        scratch_shapes=[pltpu.VMEM((HP, NST), F32), pltpu.VMEM((HP, NST), F32)],
        cost_estimate=cost(10),
        name="span_grads",
    )(me, x, g, b, c, cumr, cumc, sl, gl, dpre, dpost, packs, alog, skip)


def routing_kernel(ids_ref, gates_ref, tgt_ref, out_ref):
    experts, slots = out_ref.shape
    tokens = ids_ref.shape[1]
    expert = lax.broadcasted_iota(jnp.int32, (experts, tokens), 0)
    slot = lax.broadcasted_iota(jnp.int32, (slots, tokens), 0)
    named = [(expert == ids_ref[k : k + 1, :]).astype(F32) for k in range(2)]
    earlier = (
        lax.broadcasted_iota(jnp.int32, (tokens, tokens), 0)
        < lax.broadcasted_iota(jnp.int32, (tokens, tokens), 1)
    ).astype(BF)
    counts = dot((named[0] + named[1]).astype(BF), earlier)
    tgt_ref[...] = jnp.zeros_like(tgt_ref)
    total = jnp.zeros((experts, slots), F32)
    for k in range(2):
        position = jnp.sum(named[k] * counts, axis=0, keepdims=True).astype(jnp.int32)
        tgt_ref[k : k + 1, :] = ids_ref[k : k + 1, :] * slots + position
        placed = (slot == position).astype(BF)
        total = total + dot((named[k] * gates_ref[k : k + 1, :]).astype(BF), placed, NT)
    out_ref[...] = total.astype(out_ref.dtype)


def routing(ids, gates):
    return pl.pallas_call(
        routing_kernel,
        out_shape=(
            jax.ShapeDtypeStruct((8, ids.shape[1]), jnp.int32),
            jax.ShapeDtypeStruct((16, 16), BF),
        ),
        cost_estimate=cost(2),
        name="routing",
    )(ids, gates)


def residual_kernel(res_ref, tgt_ref, out_ref):
    for q in range(4):
        for s in range(8):
            out_ref[q, 0:128, 128 * s : 128 * (s + 1)] = res_ref[
                :, 512 * s + 128 * q : 512 * s + 128 * (q + 1)
            ]
        named = tgt_ref[...].astype(F32)
        named = jnp.concatenate([named, jnp.zeros_like(named)], axis=0).astype(BF)
        for s in range(8):
            out_ref[q, 128:144, 128 * s : 128 * (s + 1)] = named


def residual_quarters(residual, targets):
    return pl.pallas_call(
        residual_kernel,
        out_shape=jax.ShapeDtypeStruct((4, 144, 1024), BF),
        cost_estimate=cost(3),
        name="residual_quarters",
    )(residual, targets)


def rows_kernel(x_ref, w_ref, res_ref, out_ref, acc_ref):
    def step(e, carry):
        right = jnp.concatenate([w_ref[0, e % 4, e // 4], w_ref[1, e % 4, e // 4]], axis=0)
        acc_ref[...] += dot(x_ref[e], right, NT)
        return carry

    acc_ref[...] = jnp.zeros_like(acc_ref)
    lax.fori_loop(0, 16, step, 0, unroll=16)
    slot = lax.broadcasted_iota(jnp.int32, (256, 128), 0).astype(F32)
    for k in range(2):
        total = acc_ref[128 * k : 128 * (k + 1), :]
        rows = (res_ref[k, 0:128, :].astype(F32) + total).astype(BF)
        named = res_ref[k, 128:144, 0:128].astype(F32)
        picks = (slot == named[0:1, :]) | (slot == named[1:2, :])
        out_ref[:, k] = dot(picks.astype(BF), rows).astype(BF).reshape(16, 16, 256)


def expert_rows(x, weight, residual, half):
    return pl.pallas_call(
        rows_kernel,
        grid=(4,),
        in_specs=[
            pl.BlockSpec((16, 256, 256), lambda s: (0, 0, 0)),
            pl.BlockSpec((2, 4, 4, 128, 256), lambda s: (s, 0, 0, 0, 0)),
            pl.BlockSpec((2, 144, 256), lambda s: (half, 0, s)),
        ],
        out_specs=pl.BlockSpec((16, 2, 16, 256), lambda s: (0, 0, 0, s)),
        out_shape=jax.ShapeDtypeStruct((16, 2, 16, 1024), BF),
        scratch_shapes=[pltpu.VMEM((256, 256), F32)],
        compiler_params=pltpu.CompilerParams(vmem_limit_bytes=48 << 20),
        cost_estimate=cost(6),
        name="expert_rows",
    )(x, weight, residual)


def turned_kernel(w_ref, out_ref):
    for q in range(4):
        for s in range(8):
            out_ref[:, 1024 * q + 128 * s : 1024 * q + 128 * (s + 1)] = w_ref[
                :, 512 * s + 128 * q : 512 * s + 128 * (q + 1)
            ]


def turned(w):
    rows = 128
    spec = pl.BlockSpec((rows, w.shape[1]), lambda i: (i, 0))
    return pl.pallas_call(
        turned_kernel,
        grid=(w.shape[0] // rows,),
        in_specs=[spec],
        out_specs=spec,
        out_shape=jax.ShapeDtypeStruct(w.shape, w.dtype),
        cost_estimate=cost(6),
        name="turned",
    )(w)


def expert_kernel(half, at_ref, own, left, right, low, high, w_hbm, saved, gates, *rest):
    out, route_ref, xbuf, wbuf, sbuf, gbuf, obuf, up_ref, psum_ref, mixed_ref, grad_ref, sems = rest[
        -12:
    ]
    x_at, y_at = at_ref[0], at_ref[1]
    saved_copy = pltpu.make_async_copy(saved.at[y_at, :, half], sbuf.reshape(4, 128, 2, 896), sems.at[4])
    gates_copy = pltpu.make_async_copy(gates.at[y_at, :, half], gbuf.reshape(4, 128, 1), sems.at[5])
    weights = [
        pltpu.make_async_copy(
            w_hbm.at[256 * i : min(256 * (i + 1), 896), :],
            wbuf.at[256 * i : min(256 * (i + 1), 896), :],
            sems.at[i],
        )
        for i in range(4)
    ]
    copies = []
    for piece, step, first in ((own, 0, 0), (left, 3, 0), (right, 1, 0), (low, 2, 0), (high, 2, 2)):
        source = lax.rem(x_at + step, 4)
        for q in range(piece.shape[0]):
            for k in range(2):
                copies.append(
                    pltpu.make_async_copy(
                        piece.at[q, :, k],
                        xbuf.at[first + q, source, k],
                        sems.at[6 + len(copies)],
                    )
                )
    weights[0].start()
    for copy in copies:
        copy.start()
    for copy in weights[1:]:
        copy.start()
    gates_copy.start()
    saved_copy.start()
    for copy in copies:
        copy.wait()

    def tile(at, width):
        here = pl.ds(at, width)
        up_ref[:, here] = jnp.zeros((512, width), F32)

        def step(q, carry):
            piece = xbuf[q].reshape(512, 1024)
            lanes = pl.ds(pl.multiple_of(q * 1024, 1024), 1024)
            up_ref[:, here] += dot(piece, wbuf[here, lanes], NT)
            return carry

        lax.fori_loop(0, 4, step, 0)

    def later(i, carry):
        tile(pl.multiple_of(i * 256, 256), 256)
        return carry

    weights[0].wait()
    tile(0, 256)
    for copy in (weights[1], weights[2], weights[3]):
        copy.wait()
    lax.fori_loop(1, 3, later, 0)
    tile(768, 128)
    gates_copy.wait()
    saved_copy.wait()
    count = 32

    def group(j, carry):
        rows = pl.ds(pl.multiple_of(j * count, count), count)
        gate = gbuf[rows, :]
        routed = jnp.zeros((count, 128), F32)
        for n in range(7):
            lanes = slice(128 * n, 128 * (n + 1))
            mixed_ref[...] = sbuf[rows, :, lanes].reshape(2 * count, 128).astype(F32)
            gate_pre = mixed_ref[pl.ds(0, count, stride=2), :]
            up_pre = mixed_ref[pl.ds(1, count, stride=2), :]
            upstream = up_ref[rows, lanes]
            sigmoid = 1.0 / (1.0 + jnp.exp(-gate_pre))
            active = gate_pre * sigmoid
            weighted = gate * upstream
            routed = routed + active * up_pre * upstream
            grad_ref[pl.ds(0, count, stride=2), :] = (
                weighted * up_pre * sigmoid * (1.0 + gate_pre * (1.0 - sigmoid))
            )
            grad_ref[pl.ds(1, count, stride=2), :] = weighted * active
            obuf[rows, :, lanes] = grad_ref[...].astype(BF).reshape(count, 2, 128)
        psum_ref[rows, :] = routed
        return carry

    lax.fori_loop(0, 512 // count, group, 0)
    out_copy = pltpu.make_async_copy(obuf.reshape(4, 128, 2, 896), out.at[y_at, :, half], sems.at[4])
    out_copy.start()
    ones = jnp.ones((8, 128), F32)
    route_ref[...] = dot(ones, psum_ref[...], NT, precision=lax.Precision.HIGHEST)
    out_copy.wait()


def expert_grads(half, at, pieces, weight, saved, gates, before):
    own, left, right, low, high = [p.reshape(-1, 4, 2, 16, 1024) for p in pieces]
    hbm = pl.BlockSpec(memory_space=pl.ANY)
    args = [at, own, left, right, low, high, weight, saved, gates]
    if before is not None:
        args.append(before)
    return pl.pallas_call(
        functools.partial(expert_kernel, half),
        in_specs=[pl.BlockSpec(memory_space=pltpu.SMEM)] + [hbm] * (len(args) - 1),
        out_specs=[hbm, pl.BlockSpec(memory_space=pltpu.VMEM)],
        out_shape=(
            jax.ShapeDtypeStruct(saved.shape, BF),
            jax.ShapeDtypeStruct((8, 512), F32),
        ),
        scratch_shapes=[
            pltpu.VMEM((4, 4, 2, 4, 16, 1024), BF),
            pltpu.VMEM((896, 4096), BF),
            pltpu.VMEM((512, 2, 896), BF),
            pltpu.VMEM((512, 1), F32),
            pltpu.VMEM((512, 2, 896), BF),
            pltpu.VMEM((512, 896), F32),
            pltpu.VMEM((512, 128), F32),
            pltpu.VMEM((64, 128), F32),
            pltpu.VMEM((64, 128), F32),
            pltpu.SemaphoreType.DMA((40,)),
        ],
        input_output_aliases={} if before is None else {9: 0},
        compiler_params=pltpu.CompilerParams(vmem_limit_bytes=56 << 20),
        cost_estimate=cost(12),
        name="expert_grads",
    )(*args)


SEQ = ("yl", "x")
QUAD = ("yh", "zh")
MEMB = ("zl", "core")
EXP = QUAD + MEMB
BOTH = SEQ + EXP


def a2a(array, axis):
    return lax.all_to_all(array, axis, split_axis=0, concat_axis=0, tiled=True)


def shifted(array, by):
    return lax.ppermute(array, "x", [(i, (i + by) % 4) for i in range(4)])


def other_row(array):
    return lax.ppermute(array, "yl", [(0, 1), (1, 0)])


def along_x(own):
    left = shifted(own, 1)
    right = shifted(own, -1)
    low = shifted(left[:8], 1)
    high = shifted(right[8:], -1)
    return (own, left, right, low, high)


def per_device(
    gates, expert_ids, saved_pre, w_down, residual_grad, in_weight,
    ssm_in, b_proj, c_proj, step_sizes, a_log, skip_gain, ssm_grad,
):
    quarters = a2a(in_weight.reshape(4, 128, 256), QUAD)
    targets, slot_gates = routing(expert_ids.T, gates.T)
    slot_gates = a2a(slot_gates, EXP)
    residual = residual_quarters(residual_grad, targets)
    quarters, residual, ssm_in = lax.optimization_barrier((quarters, residual, ssm_in))
    weight = lax.all_gather(quarters.reshape(512, 256), SEQ + MEMB, axis=0, tiled=True)
    weight = weight.reshape(8, 4, 4, 128, 256)

    alog = a_log.reshape(4, 1)
    skip = jnp.repeat(skip_gain, HDIM).reshape(1, HP)
    *parts, pack = local_states(ssm_in, ssm_grad, b_proj, c_proj, step_sizes, alog)
    pack = jnp.concatenate([pack, jnp.pad(slot_gates, ((0, 0), (0, 112)))], axis=0)
    packs = a2a(jnp.broadcast_to(pack, (8, *pack.shape)), SEQ)
    gate_rows = packs[:, 2 * HP + 16 :, 0:16].astype(F32).reshape(2, 4, 2, 128, 1)
    residual = a2a(residual, QUAD)
    down = turned(w_down[0])

    here = lax.axis_index(SEQ).reshape(1)
    args = (here, ssm_in, ssm_grad, b_proj, c_proj, parts, packs, alog, skip)
    arrived, grads = {}, {}
    for half in (1, 0):
        x_part, bc_part, step_part = span_grads(*args, half)
        grads[half] = (bc_part, step_part)
        moved = a2a(x_part.reshape(16, 256, 256), EXP)
        rows = expert_rows(moved, weight, residual, half)
        arrived[half] = a2a(rows.reshape(16, 32, 1024), EXP)

    mine = along_x(arrived[1])
    theirs = tuple(other_row(p) for p in mine)
    partner = other_row(arrived[0])
    sets = [(1, 0, mine), (0, 0, along_x(arrived[0])), (1, 1, theirs), (0, 1, along_x(partner))]

    x_at, y_at = lax.axis_index("x"), lax.axis_index("yl")
    saved = saved_pre.reshape(2, 4, 2, 128, 2, 896)
    out, routes = None, {}
    for half, flip, pieces in sets:
        at = jnp.stack([x_at, y_at ^ flip]).astype(jnp.int32)
        out, route = expert_grads(half, at, pieces, down, saved, gate_rows, out)
        routes[half, flip] = route[0].reshape(4, 128)
    first, second = [
        jnp.stack([routes[0, flip], routes[1, flip]], axis=1).reshape(4, 256) for flip in (0, 1)
    ]
    low, high = [jnp.where(y_at == 0, a, b) for a, b in ((first, second), (second, first))]
    partial = jnp.concatenate([low, high], axis=0)
    summed = jnp.sum(a2a(partial, SEQ), axis=0)
    totals = a2a(summed.reshape(16, 16), EXP).reshape(256, 1)
    slot = lax.broadcasted_iota(jnp.int32, (256, 128), 0)
    route_grads = jnp.stack(
        [jnp.sum(jnp.where(slot == targets[k], totals, 0.0), axis=0) for k in range(2)], axis=1
    )

    both = jnp.concatenate([grads[0][0], grads[1][0]], axis=0).reshape(16, 128, 2 * NST)
    both = jnp.sum(a2a(both, EXP).astype(F32), axis=0)
    step_grads = jnp.concatenate([grads[0][1], grads[1][1]], axis=1)
    pre_grads = out.reshape(1, 2048, 2, 896)
    return (pre_grads, route_grads, both[:, :NST], both[:, NST:], step_grads)


def solution(mesh):
    split = Mesh(mesh.devices.reshape(2, 4, 2, 2, 2, 2), BOTH)
    in_specs = (
        P(BOTH, None), P(BOTH, None), P(EXP, None, None, SEQ), P(EXP, SEQ, None), P(BOTH, None),
        P(SEQ, EXP), P(SEQ, EXP), P(SEQ, None), P(SEQ, None), P(EXP, SEQ), P(EXP), P(EXP),
        P(SEQ, EXP),
    )
    out_specs = (P(EXP, None, None, SEQ), P(BOTH, None), P(BOTH, None), P(BOTH, None), P(EXP, SEQ))
    return jax.shard_map(
        per_device, mesh=split, in_specs=in_specs, out_specs=out_specs, check_vma=False
    )
```

```python
import functools
import jax
import jax.numpy as jnp
from jax import lax
from jax.experimental import pallas as pl
from jax.experimental.pallas import tpu as pltpu
from jax.sharding import Mesh
from jax.sharding import PartitionSpec as P

F32 = jnp.float32
BF = jnp.bfloat16
HEADS, HDIM, NST, L = 4, 64, 128, 128
HP = HEADS * HDIM
NT = (((1,), (1,)), ((), ()))
TN = (((0,), (0,)), ((), ()))


def dot(a, b, dims=(((1,), (0,)), ((), ())), precision=None):
    return lax.dot_general(a, b, dims, precision=precision, preferred_element_type=F32)


def cost(us):
    return pl.CostEstimate(flops=int(us * 5e8), bytes_accessed=1 << 20, transcendentals=0)


def over_heads(cols):
    low = lax.broadcasted_iota(jnp.int32, (cols.shape[0], 128), 1) < HDIM
    return jnp.concatenate(
        [jnp.where(low, cols[:, h : h + 1], cols[:, h + 1 : h + 2]) for h in (0, 2)], axis=1
    )


def head_rows(rows):
    return jnp.concatenate(
        [jnp.broadcast_to(rows[h : h + 1, :], (HDIM, NST)) for h in range(HEADS)], axis=0
    )


def states_kernel(
    x_ref, g_ref, b_ref, c_ref, step_ref, alog_ref,
    cumr_ref, cumc_ref, sl_ref, gl_ref, dpre_ref, dpost_ref, pack_ref, q_ref,
):
    spans = sl_ref.shape[0]
    q_ref[...] = jnp.zeros_like(q_ref)
    q = step_ref[...] * jnp.exp(alog_ref[...])
    for c in range(spans):
        q_ref[8 * c : 8 * c + HEADS, :] = q[:, L * c : L * (c + 1)]
    row = lax.broadcasted_iota(jnp.int32, (L, L), 0)
    col = lax.broadcasted_iota(jnp.int32, (L, L), 1)
    upper = (row <= col).astype(F32)
    cum = dot(q_ref[...], upper, precision=lax.Precision.HIGHEST)
    cumr_ref[...] = cum.reshape(spans, 8, L)
    turned = cum.T
    for c in range(spans):
        cumc_ref[c] = turned[:, 8 * c : 8 * c + 8]

    def forward(c, carry):
        state, run = carry
        sl_ref[c] = state.astype(BF)
        dpre_ref[c] = jnp.exp(-run)
        at = pl.ds(pl.multiple_of(c * L, L), L)
        cols = cumc_ref[c]
        last = jnp.broadcast_to(cumr_ref[c][:, L - 1 : L], (8, NST))
        tail = jnp.exp(jnp.minimum(cols - cols[L - 1 : L, :], 0.0))
        decayed = (x_ref[at, :].astype(F32) * over_heads(tail)).astype(BF)
        fresh = dot(decayed, b_ref[at, :], TN)
        return (head_rows(jnp.exp(-last)) * state + fresh, run + last)

    zero = (jnp.zeros((HP, NST), F32), jnp.zeros((8, NST), F32))
    state, run = lax.fori_loop(0, spans, forward, zero)
    pack_ref[0:HP, :] = state.astype(BF)
    total = jnp.exp(-run)
    high = total.astype(BF).astype(F32)
    pack_ref[2 * HP : 2 * HP + 16, :] = jnp.concatenate([high, total - high], axis=0).astype(BF)

    def backward(i, carry):
        state, run = carry
        c = spans - 1 - i
        gl_ref[c] = state.astype(BF)
        dpost_ref[c] = jnp.exp(-run)
        at = pl.ds(pl.multiple_of(c * L, L), L)
        last = jnp.broadcast_to(cumr_ref[c][:, L - 1 : L], (8, NST))
        decayed = (g_ref[at, :].astype(F32) * over_heads(jnp.exp(-cumc_ref[c]))).astype(BF)
        fresh = dot(decayed, c_ref[at, :], TN)
        return (head_rows(jnp.exp(-last)) * state + fresh, run + last)

    state, run = lax.fori_loop(0, spans, backward, zero)
    pack_ref[HP : 2 * HP, :] = state.astype(BF)


def local_states(x, g, b, c, step, alog):
    spans = x.shape[0] // L
    out = (
        jax.ShapeDtypeStruct((spans, 8, L), F32),
        jax.ShapeDtypeStruct((spans, L, 8), F32),
        jax.ShapeDtypeStruct((spans, HP, NST), BF),
        jax.ShapeDtypeStruct((spans, HP, NST), BF),
        jax.ShapeDtypeStruct((spans, 8, NST), F32),
        jax.ShapeDtypeStruct((spans, 8, NST), F32),
        jax.ShapeDtypeStruct((2 * HP + 16, NST), BF),
    )
    return pl.pallas_call(
        states_kernel,
        out_shape=out,
        scratch_shapes=[pltpu.VMEM((8 * spans, L), F32)],
        cost_estimate=cost(16),
        name="states",
    )(x, g, b, c, step, alog)


def grads_kernel(
    me_ref, x_ref, g_ref, b_ref, c_ref, cumr_ref, cumc_ref, sl_ref, gl_ref, dpre_ref, dpost_ref,
    packs_ref, alog_ref, skip_ref,
    dx_ref, bc_ref, dq_ref, sin_ref, gex_ref,
):
    count = packs_ref.shape[0]

    @pl.when(pl.program_id(0) == 0)
    def _():
        me = me_ref[0]

        def dec(s):
            both = packs_ref[s, HP : HP + 16, :].astype(F32)
            return head_rows(both[0:8] + both[8:16])

        sin_ref[...] = jnp.zeros_like(sin_ref)
        gex_ref[...] = jnp.zeros_like(gex_ref)
        for s in range(count):
            @pl.when(s < me)
            def _():
                sin_ref[...] = dec(s) * sin_ref[...] + packs_ref[s, 0:HP, :].astype(F32)
        for s in reversed(range(count)):
            @pl.when(s > me)
            def _():
                gex_ref[...] = dec(s) * gex_ref[...] + packs_ref[s, 0:HP, :].astype(F32)

    x = x_ref[...]
    g = g_ref[...]
    b = b_ref[...]
    c = c_ref[...]
    xf = x.astype(F32)
    gf = g.astype(F32)
    rows = cumr_ref[0]
    cols = cumc_ref[0]
    state = sl_ref[0].astype(F32) + head_rows(dpre_ref[0]) * sin_ref[...]
    after = gl_ref[0].astype(F32) + head_rows(dpost_ref[0]) * gex_ref[...]
    state_b = state.astype(BF)
    after_b = after.astype(BF)
    into = over_heads(jnp.exp(-cols))
    tail = over_heads(jnp.exp(jnp.minimum(cols - cols[L - 1 : L, :], 0.0)))
    g_in = (gf * into).astype(BF)
    x_tail = (xf * tail).astype(BF)
    dc = dot(g_in, state_b)
    db = dot(x_tail, after_b)
    from_after = dot(b, after_b, NT) * tail
    carried = dot(c, state_b, NT) * into
    scores = dot(c, b, NT)
    row = lax.broadcasted_iota(jnp.int32, (L, L), 0)
    col = lax.broadcasted_iota(jnp.int32, (L, L), 1)
    lower = row >= col
    before = (row < col).astype(BF)
    lower_b = lower.astype(BF)
    picks = (
        lax.broadcasted_iota(jnp.int32, (8, HP), 1) // HDIM
        == lax.broadcasted_iota(jnp.int32, (8, HP), 0)
    ).astype(BF)
    late = dot(picks, (gf * carried).astype(BF), NT)
    early = dot(picks, (xf * from_after).astype(BF), NT)
    across = jnp.sum(dot(picks, (state * after).astype(BF)), axis=1, keepdims=True)
    steps = (
        dot(late.astype(BF), lower_b)
        + dot(early.astype(BF), before)
        + across * jnp.exp(-rows[:, L - 1 : L])
    )
    mixed = jnp.zeros((L, L), F32)
    inner = []
    pieces = []
    for h in range(HEADS):
        at = slice(HDIM * h, HDIM * (h + 1))
        g_h = g[:, at]
        cross = dot(g_h, x[:, at], NT)
        decay = jnp.where(
            lower, jnp.exp(jnp.minimum(rows[h : h + 1, :] - cols[:, h : h + 1], 0.0)), 0.0
        )
        kept = decay * cross
        mixed = mixed + kept
        pieces.append(dot((decay * scores).astype(BF), g_h, TN))
        passed = dot((kept * scores).astype(BF), before)
        inner.append(jnp.sum(jnp.where(lower, passed, 0.0), axis=0, keepdims=True))
    steps = steps[0:HEADS] + jnp.concatenate(inner, axis=0)
    dq_ref[...] = -steps * jnp.exp(alog_ref[...])
    dx = jnp.concatenate(pieces, axis=1) + from_after + gf * skip_ref[...]
    dx_b = dx.astype(dx_ref.dtype)
    for q in range(dx_ref.shape[0]):
        dx_ref[q, 0, 0] = dx_b
    mixed_b = mixed.astype(BF)
    bc_ref[:, 0:NST] = (db + dot(mixed_b, c, TN)).astype(bc_ref.dtype)
    bc_ref[:, NST:] = (dc + dot(mixed_b, b)).astype(bc_ref.dtype)


def span_grads(me, x, g, b, c, parts, packs, alog, skip, half):
    cumr, cumc, sl, gl, dpre, dpost = parts
    spans = sl.shape[0] // 2
    base = half * spans
    once = lambda shape: pl.BlockSpec(shape, lambda i: (0,) * len(shape))
    lead = lambda shape: pl.BlockSpec((1, *shape), lambda i: (base + i, 0, 0))
    rows = lambda width: pl.BlockSpec((L, width), lambda i: (base + i, 0))
    return pl.pallas_call(
        grads_kernel,
        grid=(spans,),
        in_specs=[
            pl.BlockSpec(memory_space=pltpu.SMEM),
            rows(HP), rows(HP), rows(NST), rows(NST),
            lead((8, L)), lead((L, 8)), lead((HP, NST)), lead((HP, NST)),
            lead((8, NST)), lead((8, NST)),
            once(packs.shape), once(alog.shape), once(skip.shape),
        ],
        out_specs=[
            pl.BlockSpec((4, 1, 1, L, HP), lambda i: (0, i % 4, i // 4, 0, 0)),
            pl.BlockSpec((L, 2 * NST), lambda i: (i, 0)),
            pl.BlockSpec((HEADS, L), lambda i: (0, i)),
        ],
        out_shape=(
            jax.ShapeDtypeStruct((4, 4, spans // 4, L, HP), BF),
            jax.ShapeDtypeStruct((spans * L, 2 * NST), BF),
            jax.ShapeDtypeStruct((HEADS, spans * L), F32),
        ),
        scratch_shapes=[pltpu.VMEM((HP, NST), F32), pltpu.VMEM((HP, NST), F32)],
        cost_estimate=cost(10),
        name="span_grads",
    )(me, x, g, b, c, cumr, cumc, sl, gl, dpre, dpost, packs, alog, skip)


def routing_kernel(ids_ref, gates_ref, tgt_ref, out_ref):
    experts, slots = out_ref.shape
    tokens = ids_ref.shape[1]
    expert = lax.broadcasted_iota(jnp.int32, (experts, tokens), 0)
    slot = lax.broadcasted_iota(jnp.int32, (slots, tokens), 0)
    named = [(expert == ids_ref[k : k + 1, :]).astype(F32) for k in range(2)]
    earlier = (
        lax.broadcasted_iota(jnp.int32, (tokens, tokens), 0)
        < lax.broadcasted_iota(jnp.int32, (tokens, tokens), 1)
    ).astype(BF)
    counts = dot((named[0] + named[1]).astype(BF), earlier)
    tgt_ref[...] = jnp.zeros_like(tgt_ref)
    total = jnp.zeros((experts, slots), F32)
    for k in range(2):
        position = jnp.sum(named[k] * counts, axis=0, keepdims=True).astype(jnp.int32)
        tgt_ref[k : k + 1, :] = ids_ref[k : k + 1, :] * slots + position
        placed = (slot == position).astype(BF)
        total = total + dot((named[k] * gates_ref[k : k + 1, :]).astype(BF), placed, NT)
    out_ref[...] = total.astype(out_ref.dtype)


def routing(ids, gates):
    return pl.pallas_call(
        routing_kernel,
        out_shape=(
            jax.ShapeDtypeStruct((8, ids.shape[1]), jnp.int32),
            jax.ShapeDtypeStruct((16, 16), BF),
        ),
        cost_estimate=cost(2),
        name="routing",
    )(ids, gates)


def first_kernel(res_ref, tgt_ref, w_ref, out_ref):
    named = tgt_ref[...].astype(F32)
    named = jnp.concatenate([named, jnp.zeros_like(named)], axis=0).astype(BF)
    for q in range(4):
        for s in range(8):
            lanes = slice(128 * s, 128 * (s + 1))
            out_ref[q, 0:128, lanes] = res_ref[:, 512 * s + 128 * q : 512 * s + 128 * (q + 1)]
            out_ref[q, 128:144, lanes] = named
        for j in range(4):
            rows = slice(128 * q + 32 * j, 128 * q + 32 * (j + 1))
            out_ref[q, 144:176, 256 * j : 256 * (j + 1)] = w_ref[rows, :]


def first_exchange(residual, targets, weight):
    return pl.pallas_call(
        first_kernel,
        out_shape=jax.ShapeDtypeStruct((4, 176, 1024), BF),
        cost_estimate=cost(3),
        name="first_exchange",
    )(residual, targets, weight)


def rows_kernel(x_ref, w_ref, res_ref, out_ref, acc_ref):
    def step(e, carry):
        blocks = [w_ref[s, e % 4, e // 4] for s in range(2)]
        right = jnp.concatenate(
            [block[:, 256 * j : 256 * (j + 1)] for block in blocks for j in range(4)], axis=0
        )
        acc_ref[...] += dot(x_ref[e], right, NT)
        return carry

    acc_ref[...] = jnp.zeros_like(acc_ref)
    lax.fori_loop(0, 16, step, 0, unroll=16)
    slot = lax.broadcasted_iota(jnp.int32, (256, 128), 0).astype(F32)
    for k in range(2):
        total = acc_ref[128 * k : 128 * (k + 1), :]
        rows = (res_ref[k, 0:128, :].astype(F32) + total).astype(BF)
        named = res_ref[k, 128:144, 0:128].astype(F32)
        picks = (slot == named[0:1, :]) | (slot == named[1:2, :])
        out_ref[:, k] = dot(picks.astype(BF), rows).astype(BF).reshape(16, 16, 256)


def expert_rows(x, weight, residual, half):
    return pl.pallas_call(
        rows_kernel,
        grid=(4,),
        in_specs=[
            pl.BlockSpec((16, 256, 256), lambda s: (0, 0, 0)),
            pl.BlockSpec((2, 4, 4, 32, 1024), lambda s: (s, 0, 0, 0, 0)),
            pl.BlockSpec((2, 144, 256), lambda s: (half, 0, s)),
        ],
        out_specs=pl.BlockSpec((16, 2, 16, 256), lambda s: (0, 0, 0, s)),
        out_shape=jax.ShapeDtypeStruct((16, 2, 16, 1024), BF),
        scratch_shapes=[pltpu.VMEM((256, 256), F32)],
        compiler_params=pltpu.CompilerParams(vmem_limit_bytes=48 << 20),
        cost_estimate=cost(6),
        name="expert_rows",
    )(x, weight, residual)


def turned_kernel(w_ref, out_ref):
    for q in range(4):
        for s in range(8):
            out_ref[:, 1024 * q + 128 * s : 1024 * q + 128 * (s + 1)] = w_ref[
                :, 512 * s + 128 * q : 512 * s + 128 * (q + 1)
            ]


def turned(w):
    rows = 128
    spec = pl.BlockSpec((rows, w.shape[1]), lambda i: (i, 0))
    return pl.pallas_call(
        turned_kernel,
        grid=(w.shape[0] // rows,),
        in_specs=[spec],
        out_specs=spec,
        out_shape=jax.ShapeDtypeStruct(w.shape, w.dtype),
        cost_estimate=cost(6),
        name="turned",
    )(w)


def expert_kernel(half, at_ref, own, left, right, low, high, w_hbm, saved, gates, *rest):
    out, route_ref, xbuf, wbuf, sbuf, gbuf, obuf, up_ref, psum_ref, mixed_ref, grad_ref, sems = rest[
        -12:
    ]
    x_at, y_at = at_ref[0], at_ref[1]
    saved_copy = pltpu.make_async_copy(saved.at[y_at, :, half], sbuf.reshape(4, 128, 2, 896), sems.at[4])
    gates_copy = pltpu.make_async_copy(gates.at[y_at, :, half], gbuf.reshape(4, 128, 1), sems.at[5])
    weights = [
        pltpu.make_async_copy(
            w_hbm.at[256 * i : min(256 * (i + 1), 896), :],
            wbuf.at[256 * i : min(256 * (i + 1), 896), :],
            sems.at[i],
        )
        for i in range(4)
    ]
    copies = []
    for piece, step, first in ((own, 0, 0), (left, 3, 0), (right, 1, 0), (low, 2, 0), (high, 2, 2)):
        source = lax.rem(x_at + step, 4)
        for q in range(piece.shape[0]):
            for k in range(2):
                copies.append(
                    pltpu.make_async_copy(
                        piece.at[q, :, k],
                        xbuf.at[first + q, source, k],
                        sems.at[6 + len(copies)],
                    )
                )
    weights[0].start()
    for copy in copies:
        copy.start()
    for copy in weights[1:]:
        copy.start()
    gates_copy.start()
    saved_copy.start()
    for copy in copies:
        copy.wait()

    def tile(at, width):
        here = pl.ds(at, width)
        up_ref[:, here] = jnp.zeros((512, width), F32)

        def step(q, carry):
            piece = xbuf[q].reshape(512, 1024)
            lanes = pl.ds(pl.multiple_of(q * 1024, 1024), 1024)
            up_ref[:, here] += dot(piece, wbuf[here, lanes], NT)
            return carry

        lax.fori_loop(0, 4, step, 0)

    def later(i, carry):
        tile(pl.multiple_of(i * 256, 256), 256)
        return carry

    weights[0].wait()
    tile(0, 256)
    for copy in (weights[1], weights[2], weights[3]):
        copy.wait()
    lax.fori_loop(1, 3, later, 0)
    tile(768, 128)
    gates_copy.wait()
    saved_copy.wait()
    count = 32

    def group(j, carry):
        rows = pl.ds(pl.multiple_of(j * count, count), count)
        gate = gbuf[rows, :]
        routed = jnp.zeros((count, 128), F32)
        for n in range(7):
            lanes = slice(128 * n, 128 * (n + 1))
            mixed_ref[...] = sbuf[rows, :, lanes].reshape(2 * count, 128).astype(F32)
            gate_pre = mixed_ref[pl.ds(0, count, stride=2), :]
            up_pre = mixed_ref[pl.ds(1, count, stride=2), :]
            upstream = up_ref[rows, lanes]
            sigmoid = 1.0 / (1.0 + jnp.exp(-gate_pre))
            active = gate_pre * sigmoid
            weighted = gate * upstream
            routed = routed + active * up_pre * upstream
            grad_ref[pl.ds(0, count, stride=2), :] = (
                weighted * up_pre * sigmoid * (1.0 + gate_pre * (1.0 - sigmoid))
            )
            grad_ref[pl.ds(1, count, stride=2), :] = weighted * active
            obuf[rows, :, lanes] = grad_ref[...].astype(BF).reshape(count, 2, 128)
        psum_ref[rows, :] = routed
        return carry

    lax.fori_loop(0, 512 // count, group, 0)
    out_copy = pltpu.make_async_copy(obuf.reshape(4, 128, 2, 896), out.at[y_at, :, half], sems.at[4])
    out_copy.start()
    ones = jnp.ones((8, 128), F32)
    route_ref[...] = dot(ones, psum_ref[...], NT, precision=lax.Precision.HIGHEST)
    out_copy.wait()


def expert_grads(half, at, pieces, weight, saved, gates, before):
    own, left, right, low, high = [p.reshape(-1, 4, 2, 16, 1024) for p in pieces]
    hbm = pl.BlockSpec(memory_space=pl.ANY)
    args = [at, own, left, right, low, high, weight, saved, gates]
    if before is not None:
        args.append(before)
    return pl.pallas_call(
        functools.partial(expert_kernel, half),
        in_specs=[pl.BlockSpec(memory_space=pltpu.SMEM)] + [hbm] * (len(args) - 1),
        out_specs=[hbm, pl.BlockSpec(memory_space=pltpu.VMEM)],
        out_shape=(
            jax.ShapeDtypeStruct(saved.shape, BF),
            jax.ShapeDtypeStruct((8, 512), F32),
        ),
        scratch_shapes=[
            pltpu.VMEM((4, 4, 2, 4, 16, 1024), BF),
            pltpu.VMEM((896, 4096), BF),
            pltpu.VMEM((512, 2, 896), BF),
            pltpu.VMEM((512, 1), F32),
            pltpu.VMEM((512, 2, 896), BF),
            pltpu.VMEM((512, 896), F32),
            pltpu.VMEM((512, 128), F32),
            pltpu.VMEM((64, 128), F32),
            pltpu.VMEM((64, 128), F32),
            pltpu.SemaphoreType.DMA((40,)),
        ],
        input_output_aliases={} if before is None else {9: 0},
        compiler_params=pltpu.CompilerParams(vmem_limit_bytes=56 << 20),
        cost_estimate=cost(12),
        name="expert_grads",
    )(*args)


SEQ = ("yl", "x")
QUAD = ("yh", "zh")
MEMB = ("zl", "core")
EXP = QUAD + MEMB
BOTH = SEQ + EXP


def a2a(array, axis):
    return lax.all_to_all(array, axis, split_axis=0, concat_axis=0, tiled=True)


def shifted(array, by):
    return lax.ppermute(array, "x", [(i, (i + by) % 4) for i in range(4)])


def other_row(array):
    return lax.ppermute(array, "yl", [(0, 1), (1, 0)])


def along_x(own):
    return joined_x((own, shifted(own, 1), shifted(own, -1)))


def joined_x(pieces):
    own, left, right = pieces
    low = shifted(left[:8], 1)
    high = shifted(right[8:], -1)
    return (own, left, right, low, high)


def per_device(
    gates, expert_ids, saved_pre, w_down, residual_grad, in_weight,
    ssm_in, b_proj, c_proj, step_sizes, a_log, skip_gain, ssm_grad,
):
    targets, slot_gates = routing(expert_ids.T, gates.T)
    first = first_exchange(residual_grad, targets, in_weight)
    first = a2a(first, QUAD)
    weight = lax.all_gather(first[:, 144:176].reshape(128, 1024), SEQ + MEMB, axis=0, tiled=True)
    weight = weight.reshape(8, 4, 4, 32, 1024)

    alog = a_log.reshape(4, 1)
    skip = jnp.repeat(skip_gain, HDIM).reshape(1, HP)
    *parts, pack = local_states(ssm_in, ssm_grad, b_proj, c_proj, step_sizes, alog)
    first, pack = lax.optimization_barrier((first, pack))
    here = lax.axis_index(SEQ)
    later = lax.broadcasted_iota(jnp.int32, (8, HP, NST), 0) > here
    states = jnp.where(later, pack[:HP], pack[HP : 2 * HP])
    rest = jnp.concatenate([pack[2 * HP :], jnp.pad(slot_gates, ((0, 0), (0, 112)))], axis=0)
    packs = jnp.concatenate([states, jnp.broadcast_to(rest, (8, *rest.shape))], axis=1)
    packs = a2a(packs, SEQ)
    gate_rows = packs[:, HP + 16 :, 0:16].transpose(1, 0, 2)
    gate_rows = a2a(gate_rows.reshape(16, 128), EXP)
    down = turned(w_down[0])

    args = (here.reshape(1), ssm_in, ssm_grad, b_proj, c_proj, parts, packs, alog, skip)
    arrived, grads = {}, {}
    for half in (1, 0):
        x_part, bc_part, step_part = span_grads(*args, half)
        grads[half] = (bc_part, step_part)
        if half == 1:
            x_part, gate_rows = lax.optimization_barrier((x_part, gate_rows))
        moved = a2a(x_part.reshape(16, 256, 256), EXP)
        rows = expert_rows(moved, weight, first, half)
        arrived[half] = a2a(rows.reshape(16, 32, 1024), EXP)

    gate_rows = gate_rows.reshape(16, 8, 16).transpose(1, 0, 2)
    gate_rows = gate_rows.astype(F32).reshape(2, 4, 2, 128, 1)
    near = (arrived[1], shifted(arrived[1], 1), shifted(arrived[1], -1))
    across = other_row(arrived[1])
    mine = joined_x(near)
    theirs = joined_x((across, other_row(near[1]), other_row(near[2])))
    partner = other_row(arrived[0])
    sets = [(1, 0, mine), (0, 0, along_x(arrived[0])), (1, 1, theirs), (0, 1, along_x(partner))]

    x_at, y_at = lax.axis_index("x"), lax.axis_index("yl")
    saved = saved_pre.reshape(2, 4, 2, 128, 2, 896)
    out, routes = None, {}
    for half, flip, pieces in sets:
        at = jnp.stack([x_at, y_at ^ flip]).astype(jnp.int32)
        out, route = expert_grads(half, at, pieces, down, saved, gate_rows, out)
        routes[half, flip] = route[0].reshape(4, 128)
    first, second = [
        jnp.stack([routes[0, flip], routes[1, flip]], axis=1).reshape(4, 256) for flip in (0, 1)
    ]
    low, high = [jnp.where(y_at == 0, a, b) for a, b in ((first, second), (second, first))]
    partial = jnp.concatenate([low, high], axis=0)
    summed = jnp.sum(a2a(partial, SEQ), axis=0)
    totals = a2a(summed.reshape(16, 16), EXP).reshape(256, 1)
    slot = lax.broadcasted_iota(jnp.int32, (256, 128), 0)
    route_grads = jnp.stack(
        [jnp.sum(jnp.where(slot == targets[k], totals, 0.0), axis=0) for k in range(2)], axis=1
    )

    both = jnp.concatenate([grads[0][0], grads[1][0]], axis=0).reshape(16, 128, 2 * NST)
    both = jnp.sum(a2a(both, EXP).astype(F32), axis=0)
    step_grads = jnp.concatenate([grads[0][1], grads[1][1]], axis=1)
    pre_grads = out.reshape(1, 2048, 2, 896)
    return (pre_grads, route_grads, both[:, :NST], both[:, NST:], step_grads)


def solution(mesh):
    split = Mesh(mesh.devices.reshape(2, 4, 2, 2, 2, 2), BOTH)
    in_specs = (
        P(BOTH, None), P(BOTH, None), P(EXP, None, None, SEQ), P(EXP, SEQ, None), P(BOTH, None),
        P(SEQ, EXP), P(SEQ, EXP), P(SEQ, None), P(SEQ, None), P(EXP, SEQ), P(EXP), P(EXP),
        P(SEQ, EXP),
    )
    out_specs = (P(EXP, None, None, SEQ), P(BOTH, None), P(BOTH, None), P(BOTH, None), P(EXP, SEQ))

    return jax.shard_map(per_device, mesh=split, in_specs=in_specs, out_specs=out_specs, check_vma=False)
```

```python
import functools
import jax
import jax.numpy as jnp
from jax import lax
from jax.experimental import pallas as pl
from jax.experimental.pallas import tpu as pltpu
from jax.sharding import Mesh
from jax.sharding import PartitionSpec as P

F32 = jnp.float32
BF = jnp.bfloat16
HEADS, HDIM, NST, L = 4, 64, 128, 128
HP = HEADS * HDIM
NT = (((1,), (1,)), ((), ()))
TN = (((0,), (0,)), ((), ()))


def dot(a, b, dims=(((1,), (0,)), ((), ())), precision=None):
    return lax.dot_general(a, b, dims, precision=precision, preferred_element_type=F32)


def cost(us):
    return pl.CostEstimate(flops=int(us * 5e8), bytes_accessed=1 << 20, transcendentals=0)


def over_heads(cols):
    low = lax.broadcasted_iota(jnp.int32, (cols.shape[0], 128), 1) < HDIM
    return jnp.concatenate(
        [jnp.where(low, cols[:, h : h + 1], cols[:, h + 1 : h + 2]) for h in (0, 2)], axis=1
    )


def head_rows(rows):
    return jnp.concatenate(
        [jnp.broadcast_to(rows[h : h + 1, :], (HDIM, NST)) for h in range(HEADS)], axis=0
    )


def states_kernel(
    x_ref, g_ref, b_ref, c_ref, step_ref, alog_ref,
    cumr_ref, cumc_ref, sl_ref, gl_ref, dpre_ref, dpost_ref, pack_ref, q_ref,
):
    spans = sl_ref.shape[0]
    q_ref[...] = jnp.zeros_like(q_ref)
    q = step_ref[...] * jnp.exp(alog_ref[...])
    for c in range(spans):
        q_ref[8 * c : 8 * c + HEADS, :] = q[:, L * c : L * (c + 1)]
    row = lax.broadcasted_iota(jnp.int32, (L, L), 0)
    col = lax.broadcasted_iota(jnp.int32, (L, L), 1)
    upper = (row <= col).astype(F32)
    cum = dot(q_ref[...], upper, precision=lax.Precision.HIGHEST)
    cumr_ref[...] = cum.reshape(spans, 8, L)
    turned = cum.T
    for c in range(spans):
        cumc_ref[c] = turned[:, 8 * c : 8 * c + 8]

    def forward(c, carry):
        state, run = carry
        sl_ref[c] = state.astype(BF)
        dpre_ref[c] = jnp.exp(-run)
        at = pl.ds(pl.multiple_of(c * L, L), L)
        cols = cumc_ref[c]
        last = jnp.broadcast_to(cumr_ref[c][:, L - 1 : L], (8, NST))
        tail = jnp.exp(jnp.minimum(cols - cols[L - 1 : L, :], 0.0))
        decayed = (x_ref[at, :].astype(F32) * over_heads(tail)).astype(BF)
        fresh = dot(decayed, b_ref[at, :], TN)
        return (head_rows(jnp.exp(-last)) * state + fresh, run + last)

    zero = (jnp.zeros((HP, NST), F32), jnp.zeros((8, NST), F32))
    state, run = lax.fori_loop(0, spans, forward, zero)
    pack_ref[0:HP, :] = state.astype(BF)
    total = jnp.exp(-run)
    high = total.astype(BF).astype(F32)
    pack_ref[2 * HP : 2 * HP + 16, :] = jnp.concatenate([high, total - high], axis=0).astype(BF)

    def backward(i, carry):
        state, run = carry
        c = spans - 1 - i
        gl_ref[c] = state.astype(BF)
        dpost_ref[c] = jnp.exp(-run)
        at = pl.ds(pl.multiple_of(c * L, L), L)
        last = jnp.broadcast_to(cumr_ref[c][:, L - 1 : L], (8, NST))
        decayed = (g_ref[at, :].astype(F32) * over_heads(jnp.exp(-cumc_ref[c]))).astype(BF)
        fresh = dot(decayed, c_ref[at, :], TN)
        return (head_rows(jnp.exp(-last)) * state + fresh, run + last)

    state, run = lax.fori_loop(0, spans, backward, zero)
    pack_ref[HP : 2 * HP, :] = state.astype(BF)


def local_states(x, g, b, c, step, alog):
    spans = x.shape[0] // L
    out = (
        jax.ShapeDtypeStruct((spans, 8, L), F32),
        jax.ShapeDtypeStruct((spans, L, 8), F32),
        jax.ShapeDtypeStruct((spans, HP, NST), BF),
        jax.ShapeDtypeStruct((spans, HP, NST), BF),
        jax.ShapeDtypeStruct((spans, 8, NST), F32),
        jax.ShapeDtypeStruct((spans, 8, NST), F32),
        jax.ShapeDtypeStruct((2 * HP + 16, NST), BF),
    )
    return pl.pallas_call(
        states_kernel,
        out_shape=out,
        scratch_shapes=[pltpu.VMEM((8 * spans, L), F32)],
        cost_estimate=cost(16),
        name="states",
    )(x, g, b, c, step, alog)


def grads_kernel(
    me_ref, x_ref, g_ref, b_ref, c_ref, cumr_ref, cumc_ref, sl_ref, gl_ref, dpre_ref, dpost_ref,
    packs_ref, alog_ref, skip_ref,
    dx_ref, bc_ref, dq_ref, sin_ref, gex_ref,
):
    count = packs_ref.shape[0]

    @pl.when(pl.program_id(0) == 0)
    def _():
        me = me_ref[0]

        def dec(s):
            both = packs_ref[s, HP : HP + 16, :].astype(F32)
            return head_rows(both[0:8] + both[8:16])

        sin_ref[...] = jnp.zeros_like(sin_ref)
        gex_ref[...] = jnp.zeros_like(gex_ref)
        for s in range(count):
            @pl.when(s < me)
            def _():
                sin_ref[...] = dec(s) * sin_ref[...] + packs_ref[s, 0:HP, :].astype(F32)
        for s in reversed(range(count)):
            @pl.when(s > me)
            def _():
                gex_ref[...] = dec(s) * gex_ref[...] + packs_ref[s, 0:HP, :].astype(F32)

    x = x_ref[...]
    g = g_ref[...]
    b = b_ref[...]
    c = c_ref[...]
    xf = x.astype(F32)
    gf = g.astype(F32)
    rows = cumr_ref[0]
    cols = cumc_ref[0]
    state = sl_ref[0].astype(F32) + head_rows(dpre_ref[0]) * sin_ref[...]
    after = gl_ref[0].astype(F32) + head_rows(dpost_ref[0]) * gex_ref[...]
    state_b = state.astype(BF)
    after_b = after.astype(BF)
    into = over_heads(jnp.exp(-cols))
    tail = over_heads(jnp.exp(jnp.minimum(cols - cols[L - 1 : L, :], 0.0)))
    g_in = (gf * into).astype(BF)
    x_tail = (xf * tail).astype(BF)
    dc = dot(g_in, state_b)
    db = dot(x_tail, after_b)
    from_after = dot(b, after_b, NT) * tail
    carried = dot(c, state_b, NT) * into
    scores = dot(c, b, NT)
    row = lax.broadcasted_iota(jnp.int32, (L, L), 0)
    col = lax.broadcasted_iota(jnp.int32, (L, L), 1)
    lower = row >= col
    before = (row < col).astype(BF)
    lower_b = lower.astype(BF)
    picks = (
        lax.broadcasted_iota(jnp.int32, (8, HP), 1) // HDIM
        == lax.broadcasted_iota(jnp.int32, (8, HP), 0)
    ).astype(BF)
    late = dot(picks, (gf * carried).astype(BF), NT)
    early = dot(picks, (xf * from_after).astype(BF), NT)
    across = jnp.sum(dot(picks, (state * after).astype(BF)), axis=1, keepdims=True)
    steps = (
        dot(late.astype(BF), lower_b)
        + dot(early.astype(BF), before)
        + across * jnp.exp(-rows[:, L - 1 : L])
    )
    mixed = jnp.zeros((L, L), F32)
    inner = []
    pieces = []
    for h in range(HEADS):
        at = slice(HDIM * h, HDIM * (h + 1))
        g_h = g[:, at]
        cross = dot(g_h, x[:, at], NT)
        decay = jnp.where(
            lower, jnp.exp(jnp.minimum(rows[h : h + 1, :] - cols[:, h : h + 1], 0.0)), 0.0
        )
        kept = decay * cross
        mixed = mixed + kept
        pieces.append(dot((decay * scores).astype(BF), g_h, TN))
        passed = dot((kept * scores).astype(BF), before)
        inner.append(jnp.sum(jnp.where(lower, passed, 0.0), axis=0, keepdims=True))
    steps = steps[0:HEADS] + jnp.concatenate(inner, axis=0)
    dq_ref[...] = -steps * jnp.exp(alog_ref[...])
    dx = jnp.concatenate(pieces, axis=1) + from_after + gf * skip_ref[...]
    dx_b = dx.astype(dx_ref.dtype)
    for q in range(dx_ref.shape[0]):
        dx_ref[q, 0, 0] = dx_b
    mixed_b = mixed.astype(BF)
    bc_ref[:, 0:NST] = (db + dot(mixed_b, c, TN)).astype(bc_ref.dtype)
    bc_ref[:, NST:] = (dc + dot(mixed_b, b)).astype(bc_ref.dtype)


def span_grads(me, x, g, b, c, parts, packs, alog, skip, half):
    cumr, cumc, sl, gl, dpre, dpost = parts
    spans = sl.shape[0] // 2
    base = half * spans
    once = lambda shape: pl.BlockSpec(shape, lambda i: (0,) * len(shape))
    lead = lambda shape: pl.BlockSpec((1, *shape), lambda i: (base + i, 0, 0))
    rows = lambda width: pl.BlockSpec((L, width), lambda i: (base + i, 0))
    return pl.pallas_call(
        grads_kernel,
        grid=(spans,),
        in_specs=[
            pl.BlockSpec(memory_space=pltpu.SMEM),
            rows(HP), rows(HP), rows(NST), rows(NST),
            lead((8, L)), lead((L, 8)), lead((HP, NST)), lead((HP, NST)),
            lead((8, NST)), lead((8, NST)),
            once(packs.shape), once(alog.shape), once(skip.shape),
        ],
        out_specs=[
            pl.BlockSpec((4, 1, 1, L, HP), lambda i: (0, i % 4, i // 4, 0, 0)),
            pl.BlockSpec((L, 2 * NST), lambda i: (i, 0)),
            pl.BlockSpec((HEADS, L), lambda i: (0, i)),
        ],
        out_shape=(
            jax.ShapeDtypeStruct((4, 4, spans // 4, L, HP), BF),
            jax.ShapeDtypeStruct((spans * L, 2 * NST), BF),
            jax.ShapeDtypeStruct((HEADS, spans * L), F32),
        ),
        scratch_shapes=[pltpu.VMEM((HP, NST), F32), pltpu.VMEM((HP, NST), F32)],
        cost_estimate=cost(10),
        name="span_grads",
    )(me, x, g, b, c, cumr, cumc, sl, gl, dpre, dpost, packs, alog, skip)


def routing_kernel(ids_ref, gates_ref, tgt_ref, out_ref):
    experts, slots = out_ref.shape
    tokens = ids_ref.shape[1]
    expert = lax.broadcasted_iota(jnp.int32, (experts, tokens), 0)
    slot = lax.broadcasted_iota(jnp.int32, (slots, tokens), 0)
    named = [(expert == ids_ref[k : k + 1, :]).astype(F32) for k in range(2)]
    earlier = (
        lax.broadcasted_iota(jnp.int32, (tokens, tokens), 0)
        < lax.broadcasted_iota(jnp.int32, (tokens, tokens), 1)
    ).astype(BF)
    counts = dot((named[0] + named[1]).astype(BF), earlier)
    tgt_ref[...] = jnp.zeros_like(tgt_ref)
    total = jnp.zeros((experts, slots), F32)
    for k in range(2):
        position = jnp.sum(named[k] * counts, axis=0, keepdims=True).astype(jnp.int32)
        tgt_ref[k : k + 1, :] = ids_ref[k : k + 1, :] * slots + position
        placed = (slot == position).astype(BF)
        total = total + dot((named[k] * gates_ref[k : k + 1, :]).astype(BF), placed, NT)
    out_ref[...] = total.astype(out_ref.dtype)


def routing(ids, gates):
    return pl.pallas_call(
        routing_kernel,
        out_shape=(
            jax.ShapeDtypeStruct((8, ids.shape[1]), jnp.int32),
            jax.ShapeDtypeStruct((16, 16), BF),
        ),
        cost_estimate=cost(2),
        name="routing",
    )(ids, gates)


def first_kernel(res_ref, tgt_ref, w_ref, out_ref):
    named = tgt_ref[...].astype(F32)
    named = jnp.concatenate([named, jnp.zeros_like(named)], axis=0).astype(BF)
    for q in range(4):
        for s in range(8):
            lanes = slice(128 * s, 128 * (s + 1))
            out_ref[q, 0:128, lanes] = res_ref[:, 512 * s + 128 * q : 512 * s + 128 * (q + 1)]
            out_ref[q, 128:144, lanes] = named
        for j in range(4):
            rows = slice(128 * q + 32 * j, 128 * q + 32 * (j + 1))
            out_ref[q, 144:176, 256 * j : 256 * (j + 1)] = w_ref[rows, :]


def first_exchange(residual, targets, weight):
    return pl.pallas_call(
        first_kernel,
        out_shape=jax.ShapeDtypeStruct((4, 176, 1024), BF),
        cost_estimate=cost(3),
        name="first_exchange",
    )(residual, targets, weight)


def rows_kernel(x_ref, w_ref, res_ref, out_ref, acc_ref):
    def step(e, carry):
        blocks = [w_ref[s, e % 4, e // 4] for s in range(2)]
        right = jnp.concatenate(
            [block[:, 256 * j : 256 * (j + 1)] for block in blocks for j in range(4)], axis=0
        )
        acc_ref[...] += dot(x_ref[e], right, NT)
        return carry

    acc_ref[...] = jnp.zeros_like(acc_ref)
    lax.fori_loop(0, 16, step, 0, unroll=16)
    slot = lax.broadcasted_iota(jnp.int32, (256, 128), 0).astype(F32)
    for k in range(2):
        total = acc_ref[128 * k : 128 * (k + 1), :]
        rows = (res_ref[k, 0:128, :].astype(F32) + total).astype(BF)
        named = res_ref[k, 128:144, 0:128].astype(F32)
        picks = (slot == named[0:1, :]) | (slot == named[1:2, :])
        out_ref[:, k] = dot(picks.astype(BF), rows).astype(BF).reshape(16, 16, 256)


def expert_rows(x, weight, residual, half):
    return pl.pallas_call(
        rows_kernel,
        grid=(4,),
        in_specs=[
            pl.BlockSpec((16, 256, 256), lambda s: (0, 0, 0)),
            pl.BlockSpec((2, 4, 4, 32, 1024), lambda s: (s, 0, 0, 0, 0)),
            pl.BlockSpec((2, 144, 256), lambda s: (half, 0, s)),
        ],
        out_specs=pl.BlockSpec((16, 2, 16, 256), lambda s: (0, 0, 0, s)),
        out_shape=jax.ShapeDtypeStruct((16, 2, 16, 1024), BF),
        scratch_shapes=[pltpu.VMEM((256, 256), F32)],
        compiler_params=pltpu.CompilerParams(vmem_limit_bytes=48 << 20),
        cost_estimate=cost(6),
        name="expert_rows",
    )(x, weight, residual)


def turned_kernel(w_ref, out_ref):
    for q in range(4):
        for s in range(8):
            out_ref[:, 1024 * q + 128 * s : 1024 * q + 128 * (s + 1)] = w_ref[
                :, 512 * s + 128 * q : 512 * s + 128 * (q + 1)
            ]


def turned(w):
    rows = 128
    spec = pl.BlockSpec((rows, w.shape[1]), lambda i: (i, 0))
    return pl.pallas_call(
        turned_kernel,
        grid=(w.shape[0] // rows,),
        in_specs=[spec],
        out_specs=spec,
        out_shape=jax.ShapeDtypeStruct(w.shape, w.dtype),
        cost_estimate=cost(6),
        name="turned",
    )(w)


def expert_kernel(half, at_ref, own, left, right, low, high, w_hbm, saved, gates, *rest):
    out, route_ref, xbuf, wbuf, sbuf, gbuf, obuf, up_ref, psum_ref, mixed_ref, grad_ref, sems = rest[
        -12:
    ]
    x_at, y_at = at_ref[0], at_ref[1]
    saved_copy = pltpu.make_async_copy(saved.at[y_at, :, half], sbuf.reshape(4, 128, 2, 896), sems.at[4])
    gates_copy = pltpu.make_async_copy(gates.at[y_at, :, half], gbuf.reshape(4, 128, 1), sems.at[5])
    weights = [
        pltpu.make_async_copy(
            w_hbm.at[256 * i : min(256 * (i + 1), 896), :],
            wbuf.at[256 * i : min(256 * (i + 1), 896), :],
            sems.at[i],
        )
        for i in range(4)
    ]
    copies = []
    for piece, step, first in ((own, 0, 0), (left, 3, 0), (right, 1, 0), (low, 2, 0), (high, 2, 2)):
        source = lax.rem(x_at + step, 4)
        for q in range(piece.shape[0]):
            for k in range(2):
                copies.append(
                    pltpu.make_async_copy(
                        piece.at[q, :, k],
                        xbuf.at[first + q, source, k],
                        sems.at[6 + len(copies)],
                    )
                )
    weights[0].start()
    for copy in copies:
        copy.start()
    for copy in weights[1:]:
        copy.start()
    gates_copy.start()
    saved_copy.start()
    for copy in copies:
        copy.wait()

    def tile(at, width):
        here = pl.ds(at, width)
        up_ref[:, here] = jnp.zeros((512, width), F32)

        def step(q, carry):
            piece = xbuf[q].reshape(512, 1024)
            lanes = pl.ds(pl.multiple_of(q * 1024, 1024), 1024)
            up_ref[:, here] += dot(piece, wbuf[here, lanes], NT)
            return carry

        lax.fori_loop(0, 4, step, 0)

    def later(i, carry):
        tile(pl.multiple_of(i * 256, 256), 256)
        return carry

    weights[0].wait()
    tile(0, 256)
    for copy in (weights[1], weights[2], weights[3]):
        copy.wait()
    lax.fori_loop(1, 3, later, 0)
    tile(768, 128)
    gates_copy.wait()
    saved_copy.wait()
    count = 32

    def group(j, carry):
        rows = pl.ds(pl.multiple_of(j * count, count), count)
        gate = gbuf[rows, :]
        routed = jnp.zeros((count, 128), F32)
        for n in range(7):
            lanes = slice(128 * n, 128 * (n + 1))
            mixed_ref[...] = sbuf[rows, :, lanes].reshape(2 * count, 128).astype(F32)
            gate_pre = mixed_ref[pl.ds(0, count, stride=2), :]
            up_pre = mixed_ref[pl.ds(1, count, stride=2), :]
            upstream = up_ref[rows, lanes]
            sigmoid = 1.0 / (1.0 + jnp.exp(-gate_pre))
            active = gate_pre * sigmoid
            weighted = gate * upstream
            routed = routed + active * up_pre * upstream
            grad_ref[pl.ds(0, count, stride=2), :] = (
                weighted * up_pre * sigmoid * (1.0 + gate_pre * (1.0 - sigmoid))
            )
            grad_ref[pl.ds(1, count, stride=2), :] = weighted * active
            obuf[rows, :, lanes] = grad_ref[...].astype(BF).reshape(count, 2, 128)
        psum_ref[rows, :] = routed
        return carry

    lax.fori_loop(0, 512 // count, group, 0)
    out_copy = pltpu.make_async_copy(obuf.reshape(4, 128, 2, 896), out.at[y_at, :, half], sems.at[4])
    out_copy.start()
    ones = jnp.ones((8, 128), F32)
    route_ref[...] = dot(ones, psum_ref[...], NT, precision=lax.Precision.HIGHEST)
    out_copy.wait()


def expert_grads(half, at, pieces, weight, saved, gates, before):
    own, left, right, low, high = [p.reshape(-1, 4, 2, 16, 1024) for p in pieces]
    hbm = pl.BlockSpec(memory_space=pl.ANY)
    args = [at, own, left, right, low, high, weight, saved, gates]
    if before is not None:
        args.append(before)
    return pl.pallas_call(
        functools.partial(expert_kernel, half),
        in_specs=[pl.BlockSpec(memory_space=pltpu.SMEM)] + [hbm] * (len(args) - 1),
        out_specs=[hbm, pl.BlockSpec(memory_space=pltpu.VMEM)],
        out_shape=(
            jax.ShapeDtypeStruct(saved.shape, BF),
            jax.ShapeDtypeStruct((8, 512), F32),
        ),
        scratch_shapes=[
            pltpu.VMEM((4, 4, 2, 4, 16, 1024), BF),
            pltpu.VMEM((896, 4096), BF),
            pltpu.VMEM((512, 2, 896), BF),
            pltpu.VMEM((512, 1), F32),
            pltpu.VMEM((512, 2, 896), BF),
            pltpu.VMEM((512, 896), F32),
            pltpu.VMEM((512, 128), F32),
            pltpu.VMEM((64, 128), F32),
            pltpu.VMEM((64, 128), F32),
            pltpu.SemaphoreType.DMA((40,)),
        ],
        input_output_aliases={} if before is None else {9: 0},
        compiler_params=pltpu.CompilerParams(vmem_limit_bytes=56 << 20),
        cost_estimate=cost(12),
        name="expert_grads",
    )(*args)


SEQ = ("yl", "x")
QUAD = ("yh", "zh")
MEMB = ("zl", "core")
EXP = QUAD + MEMB
BOTH = SEQ + EXP


def a2a(array, axis):
    return lax.all_to_all(array, axis, split_axis=0, concat_axis=0, tiled=True)


def shifted(array, by):
    return lax.ppermute(array, "x", [(i, (i + by) % 4) for i in range(4)])


def other_row(array):
    return lax.ppermute(array, "yl", [(0, 1), (1, 0)])


def near_x(own):
    return (own, shifted(own, 1), shifted(own, -1))


def joined_x(pieces):
    own, left, right = pieces
    low = shifted(left[:8], 1)
    high = shifted(right[8:], -1)
    return (own, left, right, low, high)


def per_device(
    gates, expert_ids, saved_pre, w_down, residual_grad, in_weight,
    ssm_in, b_proj, c_proj, step_sizes, a_log, skip_gain, ssm_grad,
):
    targets, slot_gates = routing(expert_ids.T, gates.T)
    first = first_exchange(residual_grad, targets, in_weight)
    first = a2a(first, QUAD)
    weight = lax.all_gather(first[:, 144:176].reshape(128, 1024), SEQ + MEMB, axis=0, tiled=True)
    weight = weight.reshape(8, 4, 4, 32, 1024)

    alog = a_log.reshape(4, 1)
    skip = jnp.repeat(skip_gain, HDIM).reshape(1, HP)
    *parts, pack = local_states(ssm_in, ssm_grad, b_proj, c_proj, step_sizes, alog)
    first, pack = lax.optimization_barrier((first, pack))
    here = lax.axis_index(SEQ)
    later = lax.broadcasted_iota(jnp.int32, (8, HP, NST), 0) > here
    states = jnp.where(later, pack[:HP], pack[HP : 2 * HP])
    rest = jnp.concatenate([pack[2 * HP :], jnp.pad(slot_gates, ((0, 0), (0, 112)))], axis=0)
    packs = jnp.concatenate([states, jnp.broadcast_to(rest, (8, *rest.shape))], axis=1)
    packs = a2a(packs, SEQ)
    gate_rows = packs[:, HP + 16 :, 0:16].transpose(1, 0, 2)
    gate_rows = a2a(gate_rows.reshape(16, 128), EXP)
    down = turned(w_down[0])

    args = (here.reshape(1), ssm_in, ssm_grad, b_proj, c_proj, parts, packs, alog, skip)
    arrived, grads = {}, {}
    for half in (1, 0):
        x_part, bc_part, step_part = span_grads(*args, half)
        grads[half] = (bc_part, step_part)
        if half == 1:
            x_part, gate_rows = lax.optimization_barrier((x_part, gate_rows))
        moved = a2a(x_part.reshape(16, 256, 256), EXP)
        rows = expert_rows(moved, weight, first, half)
        arrived[half] = a2a(rows.reshape(16, 32, 1024), EXP)

    gate_rows = gate_rows.reshape(16, 8, 16).transpose(1, 0, 2)
    gate_rows = gate_rows.astype(F32).reshape(2, 4, 2, 128, 1)
    near = near_x(arrived[1])
    across = other_row(arrived[1])
    mine = joined_x(near)
    cross_left = other_row(near[1])
    cross_right = other_row(near[2])
    theirs = joined_x((across, cross_left, cross_right))
    partner = other_row(arrived[0])
    local = near_x(arrived[0])
    local = joined_x(local)
    partner = near_x(partner)
    partner = joined_x(partner)
    sets = [(1, 0, mine), (0, 0, local), (1, 1, theirs), (0, 1, partner)]

    x_at, y_at = lax.axis_index("x"), lax.axis_index("yl")
    saved = saved_pre.reshape(2, 4, 2, 128, 2, 896)
    out, routes = None, {}
    for half, flip, pieces in sets:
        at = jnp.stack([x_at, y_at ^ flip]).astype(jnp.int32)
        out, route = expert_grads(half, at, pieces, down, saved, gate_rows, out)
        routes[half, flip] = route[0].reshape(4, 128)
    first, second = [
        jnp.stack([routes[0, flip], routes[1, flip]], axis=1).reshape(4, 256) for flip in (0, 1)
    ]
    low, high = [jnp.where(y_at == 0, a, b) for a, b in ((first, second), (second, first))]
    partial = jnp.concatenate([low, high], axis=0)
    both = jnp.concatenate([grads[0][0], grads[1][0]], axis=0).reshape(16, 128, 2 * NST)
    both = a2a(both, EXP)
    partial, both = lax.optimization_barrier((partial, both))
    totals = a2a(partial.reshape(128, 16), BOTH).reshape(8, 16, 16)
    totals = jnp.sum(totals, axis=0).reshape(256, 1)
    slot = lax.broadcasted_iota(jnp.int32, (256, 128), 0)
    route_grads = jnp.stack(
        [jnp.sum(jnp.where(slot == targets[k], totals, 0.0), axis=0) for k in range(2)], axis=1
    )

    both = jnp.sum(both.astype(F32), axis=0)
    step_grads = jnp.concatenate([grads[0][1], grads[1][1]], axis=1)
    pre_grads = out.reshape(1, 2048, 2, 896)
    return (pre_grads, route_grads, both[:, :NST], both[:, NST:], step_grads)


def solution(mesh):
    split = Mesh(mesh.devices.reshape(2, 4, 2, 2, 2, 2), BOTH)
    in_specs = (
        P(BOTH, None), P(BOTH, None), P(EXP, None, None, SEQ), P(EXP, SEQ, None), P(BOTH, None),
        P(SEQ, EXP), P(SEQ, EXP), P(SEQ, None), P(SEQ, None), P(EXP, SEQ), P(EXP), P(EXP),
        P(SEQ, EXP),
    )
    out_specs = (P(EXP, None, None, SEQ), P(BOTH, None), P(BOTH, None), P(BOTH, None), P(EXP, SEQ))

    return jax.shard_map(per_device, mesh=split, in_specs=in_specs, out_specs=out_specs, check_vma=False)
```

```python
import functools
import jax
import jax.numpy as jnp
from jax import lax
from jax.experimental import pallas as pl
from jax.experimental.pallas import tpu as pltpu
from jax.sharding import Mesh
from jax.sharding import PartitionSpec as P

F32 = jnp.float32
BF = jnp.bfloat16
HEADS, HDIM, NST, L = 4, 64, 128, 128
HP = HEADS * HDIM
NT = (((1,), (1,)), ((), ()))
TN = (((0,), (0,)), ((), ()))


def dot(a, b, dims=(((1,), (0,)), ((), ())), precision=None):
    return lax.dot_general(a, b, dims, precision=precision, preferred_element_type=F32)


def cost(us):
    return pl.CostEstimate(flops=int(us * 5e8), bytes_accessed=1 << 20, transcendentals=0)


def over_heads(cols):
    low = lax.broadcasted_iota(jnp.int32, (cols.shape[0], 128), 1) < HDIM
    return jnp.concatenate(
        [jnp.where(low, cols[:, h : h + 1], cols[:, h + 1 : h + 2]) for h in (0, 2)], axis=1
    )


def head_rows(rows):
    return jnp.concatenate(
        [jnp.broadcast_to(rows[h : h + 1, :], (HDIM, NST)) for h in range(HEADS)], axis=0
    )


def states_kernel(
    x_ref, g_ref, b_ref, c_ref, step_ref, alog_ref,
    cumr_ref, cumc_ref, sl_ref, gl_ref, dpre_ref, dpost_ref, pack_ref, q_ref,
):
    spans = sl_ref.shape[0]
    q_ref[...] = jnp.zeros_like(q_ref)
    q = step_ref[...] * jnp.exp(alog_ref[...])
    for c in range(spans):
        q_ref[8 * c : 8 * c + HEADS, :] = q[:, L * c : L * (c + 1)]
    row = lax.broadcasted_iota(jnp.int32, (L, L), 0)
    col = lax.broadcasted_iota(jnp.int32, (L, L), 1)
    upper = (row <= col).astype(F32)
    cum = dot(q_ref[...], upper, precision=lax.Precision.HIGHEST)
    cumr_ref[...] = cum.reshape(spans, 8, L)
    turned = cum.T
    for c in range(spans):
        cumc_ref[c] = turned[:, 8 * c : 8 * c + 8]

    def spans_both(i, carry):
        state, run, after, later = carry
        c, d = i, spans - 1 - i
        sl_ref[c] = state.astype(BF)
        gl_ref[d] = after.astype(BF)
        dpre_ref[c] = jnp.exp(-run)
        dpost_ref[d] = jnp.exp(-later)
        at = pl.ds(pl.multiple_of(c * L, L), L)
        to = pl.ds(pl.multiple_of(d * L, L), L)
        cols = cumc_ref[c]
        last = jnp.broadcast_to(cumr_ref[c][:, L - 1 : L], (8, NST))
        final = jnp.broadcast_to(cumr_ref[d][:, L - 1 : L], (8, NST))
        tail = jnp.exp(jnp.minimum(cols - cols[L - 1 : L, :], 0.0))
        x_part = (x_ref[at, :].astype(F32) * over_heads(tail)).astype(BF)
        g_part = (g_ref[to, :].astype(F32) * over_heads(jnp.exp(-cumc_ref[d]))).astype(BF)
        state = head_rows(jnp.exp(-last)) * state + dot(x_part, b_ref[at, :], TN)
        after = head_rows(jnp.exp(-final)) * after + dot(g_part, c_ref[to, :], TN)
        return (state, run + last, after, later + final)

    zero = (jnp.zeros((HP, NST), F32), jnp.zeros((8, NST), F32))
    state, run, after, _ = lax.fori_loop(0, spans, spans_both, zero + zero)
    pack_ref[0:HP, :] = state.astype(BF)
    pack_ref[HP : 2 * HP, :] = after.astype(BF)
    total = jnp.exp(-run)
    high = total.astype(BF).astype(F32)
    pack_ref[2 * HP : 2 * HP + 16, :] = jnp.concatenate([high, total - high], axis=0).astype(BF)


def local_states(x, g, b, c, step, alog):
    spans = x.shape[0] // L
    out = (
        jax.ShapeDtypeStruct((spans, 8, L), F32),
        jax.ShapeDtypeStruct((spans, L, 8), F32),
        jax.ShapeDtypeStruct((spans, HP, NST), BF),
        jax.ShapeDtypeStruct((spans, HP, NST), BF),
        jax.ShapeDtypeStruct((spans, 8, NST), F32),
        jax.ShapeDtypeStruct((spans, 8, NST), F32),
        jax.ShapeDtypeStruct((2 * HP + 16, NST), BF),
    )
    return pl.pallas_call(
        states_kernel,
        out_shape=out,
        scratch_shapes=[pltpu.VMEM((8 * spans, L), F32)],
        cost_estimate=cost(16),
        name="states",
    )(x, g, b, c, step, alog)


def grads_kernel(
    me_ref, x_ref, g_ref, b_ref, c_ref, cumr_ref, cumc_ref, sl_ref, gl_ref, dpre_ref, dpost_ref,
    packs_ref, alog_ref, skip_ref,
    dx_ref, bc_ref, dq_ref, sin_ref, gex_ref,
):
    count = packs_ref.shape[0]

    @pl.when(pl.program_id(0) == 0)
    def _():
        me = me_ref[0]

        def dec(s):
            both = packs_ref[s, HP : HP + 16, :].astype(F32)
            return head_rows(both[0:8] + both[8:16])

        sin_ref[...] = jnp.zeros_like(sin_ref)
        gex_ref[...] = jnp.zeros_like(gex_ref)
        for s in range(count):
            @pl.when(s < me)
            def _():
                sin_ref[...] = dec(s) * sin_ref[...] + packs_ref[s, 0:HP, :].astype(F32)
        for s in reversed(range(count)):
            @pl.when(s > me)
            def _():
                gex_ref[...] = dec(s) * gex_ref[...] + packs_ref[s, 0:HP, :].astype(F32)

    x = x_ref[...]
    g = g_ref[...]
    b = b_ref[...]
    c = c_ref[...]
    xf = x.astype(F32)
    gf = g.astype(F32)
    rows = cumr_ref[0]
    cols = cumc_ref[0]
    state = sl_ref[0].astype(F32) + head_rows(dpre_ref[0]) * sin_ref[...]
    after = gl_ref[0].astype(F32) + head_rows(dpost_ref[0]) * gex_ref[...]
    state_b = state.astype(BF)
    after_b = after.astype(BF)
    into = over_heads(jnp.exp(-cols))
    tail = over_heads(jnp.exp(jnp.minimum(cols - cols[L - 1 : L, :], 0.0)))
    g_in = (gf * into).astype(BF)
    x_tail = (xf * tail).astype(BF)
    dc = dot(g_in, state_b)
    db = dot(x_tail, after_b)
    from_after = dot(b, after_b, NT) * tail
    carried = dot(c, state_b, NT) * into
    scores = dot(c, b, NT)
    row = lax.broadcasted_iota(jnp.int32, (L, L), 0)
    col = lax.broadcasted_iota(jnp.int32, (L, L), 1)
    lower = row >= col
    before = (row < col).astype(BF)
    lower_b = lower.astype(BF)
    picks = (
        lax.broadcasted_iota(jnp.int32, (8, HP), 1) // HDIM
        == lax.broadcasted_iota(jnp.int32, (8, HP), 0)
    ).astype(BF)
    late = dot(picks, (gf * carried).astype(BF), NT)
    early = dot(picks, (xf * from_after).astype(BF), NT)
    across = jnp.sum(dot(picks, (state * after).astype(BF)), axis=1, keepdims=True)
    steps = (
        dot(late.astype(BF), lower_b)
        + dot(early.astype(BF), before)
        + across * jnp.exp(-rows[:, L - 1 : L])
    )
    mixed = jnp.zeros((L, L), F32)
    inner = []
    pieces = []
    for h in range(HEADS):
        at = slice(HDIM * h, HDIM * (h + 1))
        g_h = g[:, at]
        cross = dot(g_h, x[:, at], NT)
        decay = jnp.where(
            lower, jnp.exp(jnp.minimum(rows[h : h + 1, :] - cols[:, h : h + 1], 0.0)), 0.0
        )
        kept = decay * cross
        mixed = mixed + kept
        pieces.append(dot((decay * scores).astype(BF), g_h, TN))
        passed = dot((kept * scores).astype(BF), before)
        inner.append(jnp.sum(jnp.where(lower, passed, 0.0), axis=0, keepdims=True))
    steps = steps[0:HEADS] + jnp.concatenate(inner, axis=0)
    dq_ref[...] = -steps * jnp.exp(alog_ref[...])
    dx = jnp.concatenate(pieces, axis=1) + from_after + gf * skip_ref[...]
    dx_b = dx.astype(dx_ref.dtype)
    for q in range(dx_ref.shape[0]):
        dx_ref[q, 0, 0] = dx_b
    mixed_b = mixed.astype(BF)
    bc_ref[:, 0:NST] = (db + dot(mixed_b, c, TN)).astype(bc_ref.dtype)
    bc_ref[:, NST:] = (dc + dot(mixed_b, b)).astype(bc_ref.dtype)


def span_grads(me, x, g, b, c, parts, packs, alog, skip, half):
    cumr, cumc, sl, gl, dpre, dpost = parts
    spans = sl.shape[0] // 2
    base = half * spans
    once = lambda shape: pl.BlockSpec(shape, lambda i: (0,) * len(shape))
    lead = lambda shape: pl.BlockSpec((1, *shape), lambda i: (base + i, 0, 0))
    rows = lambda width: pl.BlockSpec((L, width), lambda i: (base + i, 0))
    return pl.pallas_call(
        grads_kernel,
        grid=(spans,),
        in_specs=[
            pl.BlockSpec(memory_space=pltpu.SMEM),
            rows(HP), rows(HP), rows(NST), rows(NST),
            lead((8, L)), lead((L, 8)), lead((HP, NST)), lead((HP, NST)),
            lead((8, NST)), lead((8, NST)),
            once(packs.shape), once(alog.shape), once(skip.shape),
        ],
        out_specs=[
            pl.BlockSpec((4, 1, 1, L, HP), lambda i: (0, i % 4, i // 4, 0, 0)),
            pl.BlockSpec((L, 2 * NST), lambda i: (i, 0)),
            pl.BlockSpec((HEADS, L), lambda i: (0, i)),
        ],
        out_shape=(
            jax.ShapeDtypeStruct((4, 4, spans // 4, L, HP), BF),
            jax.ShapeDtypeStruct((spans * L, 2 * NST), BF),
            jax.ShapeDtypeStruct((HEADS, spans * L), F32),
        ),
        scratch_shapes=[pltpu.VMEM((HP, NST), F32), pltpu.VMEM((HP, NST), F32)],
        cost_estimate=cost(10),
        name="span_grads",
    )(me, x, g, b, c, cumr, cumc, sl, gl, dpre, dpost, packs, alog, skip)


def routing_kernel(ids_ref, gates_ref, tgt_ref, out_ref):
    experts, slots = out_ref.shape
    tokens = ids_ref.shape[1]
    expert = lax.broadcasted_iota(jnp.int32, (experts, tokens), 0)
    slot = lax.broadcasted_iota(jnp.int32, (slots, tokens), 0)
    named = [(expert == ids_ref[k : k + 1, :]).astype(F32) for k in range(2)]
    earlier = (
        lax.broadcasted_iota(jnp.int32, (tokens, tokens), 0)
        < lax.broadcasted_iota(jnp.int32, (tokens, tokens), 1)
    ).astype(BF)
    counts = dot((named[0] + named[1]).astype(BF), earlier)
    tgt_ref[...] = jnp.zeros_like(tgt_ref)
    total = jnp.zeros((experts, slots), F32)
    for k in range(2):
        position = jnp.sum(named[k] * counts, axis=0, keepdims=True).astype(jnp.int32)
        tgt_ref[k : k + 1, :] = ids_ref[k : k + 1, :] * slots + position
        placed = (slot == position).astype(BF)
        total = total + dot((named[k] * gates_ref[k : k + 1, :]).astype(BF), placed, NT)
    out_ref[...] = total.astype(out_ref.dtype)


def routing(ids, gates):
    return pl.pallas_call(
        routing_kernel,
        out_shape=(
            jax.ShapeDtypeStruct((8, ids.shape[1]), jnp.int32),
            jax.ShapeDtypeStruct((16, 16), BF),
        ),
        cost_estimate=cost(2),
        name="routing",
    )(ids, gates)


def first_kernel(res_ref, tgt_ref, w_ref, out_ref):
    named = tgt_ref[...].astype(F32)
    named = jnp.concatenate([named, jnp.zeros_like(named)], axis=0).astype(BF)
    for q in range(4):
        for s in range(8):
            lanes = slice(128 * s, 128 * (s + 1))
            out_ref[q, 0:128, lanes] = res_ref[:, 512 * s + 128 * q : 512 * s + 128 * (q + 1)]
            out_ref[q, 128:144, lanes] = named
        for j in range(4):
            rows = slice(128 * q + 32 * j, 128 * q + 32 * (j + 1))
            out_ref[q, 144:176, 256 * j : 256 * (j + 1)] = w_ref[rows, :]


def first_exchange(residual, targets, weight):
    return pl.pallas_call(
        first_kernel,
        out_shape=jax.ShapeDtypeStruct((4, 176, 1024), BF),
        cost_estimate=cost(3),
        name="first_exchange",
    )(residual, targets, weight)


def rows_kernel(x_ref, w_ref, res_ref, out_ref, acc_ref):
    def step(e, carry):
        blocks = [w_ref[s, e % 4, e // 4] for s in range(2)]
        right = jnp.concatenate(
            [block[:, 256 * j : 256 * (j + 1)] for block in blocks for j in range(4)], axis=0
        )
        acc_ref[...] += dot(x_ref[e], right, NT)
        return carry

    acc_ref[...] = jnp.zeros_like(acc_ref)
    lax.fori_loop(0, 16, step, 0, unroll=16)
    slot = lax.broadcasted_iota(jnp.int32, (256, 128), 0).astype(F32)
    for k in range(2):
        total = acc_ref[128 * k : 128 * (k + 1), :]
        rows = (res_ref[k, 0:128, :].astype(F32) + total).astype(BF)
        named = res_ref[k, 128:144, 0:128].astype(F32)
        picks = (slot == named[0:1, :]) | (slot == named[1:2, :])
        out_ref[:, k] = dot(picks.astype(BF), rows).astype(BF).reshape(16, 16, 256)


def expert_rows(x, weight, residual, half):
    return pl.pallas_call(
        rows_kernel,
        grid=(4,),
        in_specs=[
            pl.BlockSpec((16, 256, 256), lambda s: (0, 0, 0)),
            pl.BlockSpec((2, 4, 4, 32, 1024), lambda s: (s, 0, 0, 0, 0)),
            pl.BlockSpec((2, 144, 256), lambda s: (half, 0, s)),
        ],
        out_specs=pl.BlockSpec((16, 2, 16, 256), lambda s: (0, 0, 0, s)),
        out_shape=jax.ShapeDtypeStruct((16, 2, 16, 1024), BF),
        scratch_shapes=[pltpu.VMEM((256, 256), F32)],
        compiler_params=pltpu.CompilerParams(vmem_limit_bytes=48 << 20),
        cost_estimate=cost(6),
        name="expert_rows",
    )(x, weight, residual)


def turned_kernel(w_ref, out_ref):
    for q in range(4):
        for s in range(8):
            out_ref[:, 1024 * q + 128 * s : 1024 * q + 128 * (s + 1)] = w_ref[
                :, 512 * s + 128 * q : 512 * s + 128 * (q + 1)
            ]


def turned(w):
    rows = 128
    spec = pl.BlockSpec((rows, w.shape[1]), lambda i: (i, 0))
    return pl.pallas_call(
        turned_kernel,
        grid=(w.shape[0] // rows,),
        in_specs=[spec],
        out_specs=spec,
        out_shape=jax.ShapeDtypeStruct(w.shape, w.dtype),
        cost_estimate=cost(6),
        name="turned",
    )(w)


def expert_kernel(half, at_ref, own, left, right, low, high, w_hbm, saved, gates, *rest):
    out, route_ref, xbuf, wbuf, sbuf, gbuf, obuf, up_ref, psum_ref, mixed_ref, grad_ref, sems, x_sems = (
        rest[-13:]
    )
    x_at, y_at = at_ref[0], at_ref[1]
    saved_copy = pltpu.make_async_copy(saved.at[y_at, :, half], sbuf.reshape(4, 128, 2, 896), sems.at[4])
    gates_copy = pltpu.make_async_copy(gates.at[y_at, :, half], gbuf.reshape(4, 128, 1), sems.at[5])
    lanes_of = lambda q: pl.ds(pl.multiple_of(q * 1024, 1024), 1024)
    weights_of = lambda q: pltpu.make_async_copy(
        w_hbm.at[:, lanes_of(q)], wbuf.at[:, lanes_of(q)], sems.at[q]
    )
    sources = [lax.rem(x_at + step, 4) for step in (0, 3, 1, 2)]
    for q in range(4):
        far = (low, q) if q < 2 else (high, q - 2)
        for j, (piece, at) in enumerate(((own, q), (left, q), (right, q), far)):
            for k in range(2):
                pltpu.make_async_copy(
                    piece.at[at, :, k], xbuf.at[q, sources[j], k], x_sems.at[q, j, k]
                ).start()
        weights_of(q).start()
    gates_copy.start()
    saved_copy.start()
    up_ref[...] = jnp.zeros_like(up_ref)

    def by_quarter(q, carry):
        for j in range(4):
            for k in range(2):
                pltpu.make_async_copy(
                    own.at[q, :, k], xbuf.at[q, sources[j], k], x_sems.at[q, j, k]
                ).wait()
        weights_of(q).wait()

        def tile(at, width):
            here = pl.ds(at, width)
            piece = xbuf[q].reshape(512, 1024)
            up_ref[:, here] += dot(piece, wbuf[here, lanes_of(q)], NT)

        def wide(i, carry):
            tile(pl.multiple_of(i * 256, 256), 256)
            return carry

        lax.fori_loop(0, 3, wide, 0)
        tile(768, 128)
        return carry

    lax.fori_loop(0, 4, by_quarter, 0)
    gates_copy.wait()
    saved_copy.wait()
    count = 32

    def group(j, carry):
        rows = pl.ds(pl.multiple_of(j * count, count), count)
        gate = gbuf[rows, :]
        routed = jnp.zeros((count, 128), F32)
        for n in range(7):
            lanes = slice(128 * n, 128 * (n + 1))
            mixed_ref[...] = sbuf[rows, :, lanes].reshape(2 * count, 128).astype(F32)
            gate_pre = mixed_ref[pl.ds(0, count, stride=2), :]
            up_pre = mixed_ref[pl.ds(1, count, stride=2), :]
            upstream = up_ref[rows, lanes]
            sigmoid = 1.0 / (1.0 + jnp.exp(-gate_pre))
            active = gate_pre * sigmoid
            weighted = gate * upstream
            routed = routed + active * up_pre * upstream
            grad_ref[pl.ds(0, count, stride=2), :] = (
                weighted * up_pre * sigmoid * (1.0 + gate_pre * (1.0 - sigmoid))
            )
            grad_ref[pl.ds(1, count, stride=2), :] = weighted * active
            obuf[rows, :, lanes] = grad_ref[...].astype(BF).reshape(count, 2, 128)
        psum_ref[rows, :] = routed
        return carry

    def out_of(j):
        rows = pl.ds(pl.multiple_of(j * 128, 128), 128)
        return pltpu.make_async_copy(obuf.at[rows], out.at[y_at, j, half], sems.at[6 + j])

    def block(j, carry):
        lax.fori_loop(j * (128 // count), (j + 1) * (128 // count), group, 0)
        out_of(j).start()
        return carry

    lax.fori_loop(0, 4, block, 0)
    ones = jnp.ones((8, 128), F32)
    route_ref[...] = dot(ones, psum_ref[...], NT, precision=lax.Precision.HIGHEST)
    for j in range(4):
        out_of(j).wait()


def expert_grads(half, at, pieces, weight, saved, gates, before):
    own, left, right, low, high = [p.reshape(-1, 4, 2, 16, 1024) for p in pieces]
    hbm = pl.BlockSpec(memory_space=pl.ANY)
    args = [at, own, left, right, low, high, weight, saved, gates]
    if before is not None:
        args.append(before)
    return pl.pallas_call(
        functools.partial(expert_kernel, half),
        in_specs=[pl.BlockSpec(memory_space=pltpu.SMEM)] + [hbm] * (len(args) - 1),
        out_specs=[hbm, pl.BlockSpec(memory_space=pltpu.VMEM)],
        out_shape=(
            jax.ShapeDtypeStruct(saved.shape, BF),
            jax.ShapeDtypeStruct((8, 512), F32),
        ),
        scratch_shapes=[
            pltpu.VMEM((4, 4, 2, 4, 16, 1024), BF),
            pltpu.VMEM((896, 4096), BF),
            pltpu.VMEM((512, 2, 896), BF),
            pltpu.VMEM((512, 1), F32),
            pltpu.VMEM((512, 2, 896), BF),
            pltpu.VMEM((512, 896), F32),
            pltpu.VMEM((512, 128), F32),
            pltpu.VMEM((64, 128), F32),
            pltpu.VMEM((64, 128), F32),
            pltpu.SemaphoreType.DMA((12,)),
            pltpu.SemaphoreType.DMA((4, 4, 2)),
        ],
        input_output_aliases={} if before is None else {9: 0},
        compiler_params=pltpu.CompilerParams(vmem_limit_bytes=56 << 20),
        cost_estimate=cost(12),
        name="expert_grads",
    )(*args)


SEQ = ("yl", "x")
QUAD = ("yh", "zh")
MEMB = ("zl", "core")
EXP = QUAD + MEMB
BOTH = SEQ + EXP


def a2a(array, axis):
    return lax.all_to_all(array, axis, split_axis=0, concat_axis=0, tiled=True)


def shifted(array, by):
    return lax.ppermute(array, "x", [(i, (i + by) % 4) for i in range(4)])


def other_row(array):
    return lax.ppermute(array, "yl", [(0, 1), (1, 0)])


def near_x(own):
    return (own, shifted(own, 1), shifted(own, -1))


def joined_x(pieces):
    own, left, right = pieces
    low = shifted(left[:8], 1)
    high = shifted(right[8:], -1)
    return (own, left, right, low, high)


def per_device(
    gates, expert_ids, saved_pre, w_down, residual_grad, in_weight,
    ssm_in, b_proj, c_proj, step_sizes, a_log, skip_gain, ssm_grad,
):
    targets, slot_gates = routing(expert_ids.T, gates.T)
    first = first_exchange(residual_grad, targets, in_weight)
    first = a2a(first, QUAD)
    weight = lax.all_gather(first[:, 144:176].reshape(128, 1024), SEQ + MEMB, axis=0, tiled=True)
    weight = weight.reshape(8, 4, 4, 32, 1024)

    alog = a_log.reshape(4, 1)
    skip = jnp.repeat(skip_gain, HDIM).reshape(1, HP)
    *parts, pack = local_states(ssm_in, ssm_grad, b_proj, c_proj, step_sizes, alog)
    first, pack = lax.optimization_barrier((first, pack))
    here = lax.axis_index(SEQ)
    later = lax.broadcasted_iota(jnp.int32, (8, HP, NST), 0) > here
    states = jnp.where(later, pack[:HP], pack[HP : 2 * HP])
    rest = jnp.concatenate([pack[2 * HP :], jnp.pad(slot_gates, ((0, 0), (0, 112)))], axis=0)
    packs = jnp.concatenate([states, jnp.broadcast_to(rest, (8, *rest.shape))], axis=1)
    packs = a2a(packs, SEQ)
    gate_rows = packs[:, HP + 16 :, 0:16].transpose(1, 0, 2)
    gate_rows = a2a(gate_rows.reshape(16, 128), EXP)
    down = turned(w_down[0])

    args = (here.reshape(1), ssm_in, ssm_grad, b_proj, c_proj, parts, packs, alog, skip)
    arrived, grads = {}, {}
    for half in (1, 0):
        x_part, bc_part, step_part = span_grads(*args, half)
        grads[half] = (bc_part, step_part)
        if half == 1:
            x_part, gate_rows = lax.optimization_barrier((x_part, gate_rows))
        moved = a2a(x_part.reshape(16, 256, 256), EXP)
        rows = expert_rows(moved, weight, first, half)
        arrived[half] = a2a(rows.reshape(16, 32, 1024), EXP)

    gate_rows = gate_rows.reshape(16, 8, 16).transpose(1, 0, 2)
    gate_rows = gate_rows.astype(F32).reshape(2, 4, 2, 128, 1)
    near = near_x(arrived[1])
    across = other_row(arrived[1])
    mine = joined_x(near)
    cross_left = other_row(near[1])
    cross_right = other_row(near[2])
    theirs = joined_x((across, cross_left, cross_right))
    partner = other_row(arrived[0])
    local = near_x(arrived[0])
    local = joined_x(local)
    partner = near_x(partner)
    partner = joined_x(partner)
    sets = [(1, 0, mine), (0, 0, local), (1, 1, theirs), (0, 1, partner)]

    x_at, y_at = lax.axis_index("x"), lax.axis_index("yl")
    saved = saved_pre.reshape(2, 4, 2, 128, 2, 896)
    out, routes = None, {}
    for half, flip, pieces in sets:
        at = jnp.stack([x_at, y_at ^ flip]).astype(jnp.int32)
        out, route = expert_grads(half, at, pieces, down, saved, gate_rows, out)
        routes[half, flip] = route[0].reshape(4, 128)
    first, second = [
        jnp.stack([routes[0, flip], routes[1, flip]], axis=1).reshape(4, 256) for flip in (0, 1)
    ]
    low, high = [jnp.where(y_at == 0, a, b) for a, b in ((first, second), (second, first))]
    partial = jnp.concatenate([low, high], axis=0)
    both = jnp.concatenate([grads[0][0], grads[1][0]], axis=0).reshape(16, 128, 2 * NST)
    both = a2a(both, EXP)
    partial, both = lax.optimization_barrier((partial, both))
    totals = a2a(partial.reshape(128, 16), BOTH).reshape(8, 16, 16)
    totals = jnp.sum(totals, axis=0).reshape(256, 1)
    slot = lax.broadcasted_iota(jnp.int32, (256, 128), 0)
    route_grads = jnp.stack(
        [jnp.sum(jnp.where(slot == targets[k], totals, 0.0), axis=0) for k in range(2)], axis=1
    )

    both = jnp.sum(both.astype(F32), axis=0)
    step_grads = jnp.concatenate([grads[0][1], grads[1][1]], axis=1)
    pre_grads = out.reshape(1, 2048, 2, 896)
    return (pre_grads, route_grads, both[:, :NST], both[:, NST:], step_grads)


def solution(mesh):
    split = Mesh(mesh.devices.reshape(2, 4, 2, 2, 2, 2), BOTH)
    in_specs = (
        P(BOTH, None), P(BOTH, None), P(EXP, None, None, SEQ), P(EXP, SEQ, None), P(BOTH, None),
        P(SEQ, EXP), P(SEQ, EXP), P(SEQ, None), P(SEQ, None), P(EXP, SEQ), P(EXP), P(EXP),
        P(SEQ, EXP),
    )
    out_specs = (P(EXP, None, None, SEQ), P(BOTH, None), P(BOTH, None), P(BOTH, None), P(EXP, SEQ))

    return jax.shard_map(per_device, mesh=split, in_specs=in_specs, out_specs=out_specs, check_vma=False)
```

```python
import functools
import jax
import jax.numpy as jnp
from jax import lax
from jax.experimental import pallas as pl
from jax.experimental.pallas import tpu as pltpu
from jax.sharding import Mesh
from jax.sharding import PartitionSpec as P

F32 = jnp.float32
BF = jnp.bfloat16
HEADS, HDIM, NST, L = 4, 64, 128, 128
HP = HEADS * HDIM
NT = (((1,), (1,)), ((), ()))
TN = (((0,), (0,)), ((), ()))


def dot(a, b, dims=(((1,), (0,)), ((), ())), precision=None):
    return lax.dot_general(a, b, dims, precision=precision, preferred_element_type=F32)


def cost(us):
    return pl.CostEstimate(flops=int(us * 5e8), bytes_accessed=1 << 20, transcendentals=0)


def over_heads(cols):
    low = lax.broadcasted_iota(jnp.int32, (cols.shape[0], 128), 1) < HDIM
    return jnp.concatenate(
        [jnp.where(low, cols[:, h : h + 1], cols[:, h + 1 : h + 2]) for h in (0, 2)], axis=1
    )


def head_rows(rows):
    return jnp.concatenate(
        [jnp.broadcast_to(rows[h : h + 1, :], (HDIM, NST)) for h in range(HEADS)], axis=0
    )


def states_kernel(
    x_ref, g_ref, b_ref, c_ref, step_ref, alog_ref,
    cumr_ref, cumc_ref, sl_ref, gl_ref, dpre_ref, dpost_ref, pack_ref, q_ref,
):
    spans = sl_ref.shape[0]
    q_ref[...] = jnp.zeros_like(q_ref)
    q = step_ref[...] * jnp.exp(alog_ref[...])
    for c in range(spans):
        q_ref[8 * c : 8 * c + HEADS, :] = q[:, L * c : L * (c + 1)]
    row = lax.broadcasted_iota(jnp.int32, (L, L), 0)
    col = lax.broadcasted_iota(jnp.int32, (L, L), 1)
    upper = (row <= col).astype(F32)
    cum = dot(q_ref[...], upper, precision=lax.Precision.HIGHEST)
    cumr_ref[...] = cum.reshape(spans, 8, L)
    turned = cum.T
    for c in range(spans):
        cumc_ref[c] = turned[:, 8 * c : 8 * c + 8]

    def spans_both(i, carry):
        state, run, after, later = carry
        c, d = i, spans - 1 - i
        sl_ref[c] = state.astype(BF)
        gl_ref[d] = after.astype(BF)
        dpre_ref[c] = jnp.exp(-run)
        dpost_ref[d] = jnp.exp(-later)
        at = pl.ds(pl.multiple_of(c * L, L), L)
        to = pl.ds(pl.multiple_of(d * L, L), L)
        cols = cumc_ref[c]
        last = jnp.broadcast_to(cumr_ref[c][:, L - 1 : L], (8, NST))
        final = jnp.broadcast_to(cumr_ref[d][:, L - 1 : L], (8, NST))
        tail = jnp.exp(jnp.minimum(cols - cols[L - 1 : L, :], 0.0))
        x_part = (x_ref[at, :].astype(F32) * over_heads(tail)).astype(BF)
        g_part = (g_ref[to, :].astype(F32) * over_heads(jnp.exp(-cumc_ref[d]))).astype(BF)
        state = head_rows(jnp.exp(-last)) * state + dot(x_part, b_ref[at, :], TN)
        after = head_rows(jnp.exp(-final)) * after + dot(g_part, c_ref[to, :], TN)
        return (state, run + last, after, later + final)

    zero = (jnp.zeros((HP, NST), F32), jnp.zeros((8, NST), F32))
    state, run, after, _ = lax.fori_loop(0, spans, spans_both, zero + zero)
    pack_ref[0:HP, :] = state.astype(BF)
    pack_ref[HP : 2 * HP, :] = after.astype(BF)
    total = jnp.exp(-run)
    high = total.astype(BF).astype(F32)
    pack_ref[2 * HP : 2 * HP + 16, :] = jnp.concatenate([high, total - high], axis=0).astype(BF)


def local_states(x, g, b, c, step, alog):
    spans = x.shape[0] // L
    out = (
        jax.ShapeDtypeStruct((spans, 8, L), F32),
        jax.ShapeDtypeStruct((spans, L, 8), F32),
        jax.ShapeDtypeStruct((spans, HP, NST), BF),
        jax.ShapeDtypeStruct((spans, HP, NST), BF),
        jax.ShapeDtypeStruct((spans, 8, NST), F32),
        jax.ShapeDtypeStruct((spans, 8, NST), F32),
        jax.ShapeDtypeStruct((2 * HP + 16, NST), BF),
    )
    return pl.pallas_call(
        states_kernel,
        out_shape=out,
        scratch_shapes=[pltpu.VMEM((8 * spans, L), F32)],
        cost_estimate=cost(16),
        name="states",
    )(x, g, b, c, step, alog)


def grads_kernel(
    me_ref, x_ref, g_ref, b_ref, c_ref, cumr_ref, cumc_ref, sl_ref, gl_ref, dpre_ref, dpost_ref,
    packs_ref, alog_ref, skip_ref,
    dx_ref, bc_ref, dq_ref, sin_ref, gex_ref,
):
    count = packs_ref.shape[0]

    @pl.when(pl.program_id(0) == 0)
    def _():
        me = me_ref[0]

        def dec(s):
            both = packs_ref[s, HP : HP + 16, :].astype(F32)
            return head_rows(both[0:8] + both[8:16])

        sin_ref[...] = jnp.zeros_like(sin_ref)
        gex_ref[...] = jnp.zeros_like(gex_ref)
        for s in range(count):
            @pl.when(s < me)
            def _():
                sin_ref[...] = dec(s) * sin_ref[...] + packs_ref[s, 0:HP, :].astype(F32)
        for s in reversed(range(count)):
            @pl.when(s > me)
            def _():
                gex_ref[...] = dec(s) * gex_ref[...] + packs_ref[s, 0:HP, :].astype(F32)

    x = x_ref[...]
    g = g_ref[...]
    b = b_ref[...]
    c = c_ref[...]
    xf = x.astype(F32)
    gf = g.astype(F32)
    rows = cumr_ref[0]
    cols = cumc_ref[0]
    state = sl_ref[0].astype(F32) + head_rows(dpre_ref[0]) * sin_ref[...]
    after = gl_ref[0].astype(F32) + head_rows(dpost_ref[0]) * gex_ref[...]
    state_b = state.astype(BF)
    after_b = after.astype(BF)
    into = over_heads(jnp.exp(-cols))
    tail = over_heads(jnp.exp(jnp.minimum(cols - cols[L - 1 : L, :], 0.0)))
    g_in = (gf * into).astype(BF)
    x_tail = (xf * tail).astype(BF)
    dc = dot(g_in, state_b)
    db = dot(x_tail, after_b)
    from_after = dot(b, after_b, NT) * tail
    carried = dot(c, state_b, NT) * into
    scores = dot(c, b, NT)
    row = lax.broadcasted_iota(jnp.int32, (L, L), 0)
    col = lax.broadcasted_iota(jnp.int32, (L, L), 1)
    lower = row >= col
    before = (row < col).astype(BF)
    lower_b = lower.astype(BF)
    picks = (
        lax.broadcasted_iota(jnp.int32, (8, HP), 1) // HDIM
        == lax.broadcasted_iota(jnp.int32, (8, HP), 0)
    ).astype(BF)
    late = dot(picks, (gf * carried).astype(BF), NT)
    early = dot(picks, (xf * from_after).astype(BF), NT)
    across = jnp.sum(dot(picks, (state * after).astype(BF)), axis=1, keepdims=True)
    steps = (
        dot(late.astype(BF), lower_b)
        + dot(early.astype(BF), before)
        + across * jnp.exp(-rows[:, L - 1 : L])
    )
    mixed = jnp.zeros((L, L), F32)
    inner = []
    pieces = []
    for h in range(HEADS):
        at = slice(HDIM * h, HDIM * (h + 1))
        g_h = g[:, at]
        cross = dot(g_h, x[:, at], NT)
        decay = jnp.where(
            lower, jnp.exp(jnp.minimum(rows[h : h + 1, :] - cols[:, h : h + 1], 0.0)), 0.0
        )
        kept = decay * cross
        mixed = mixed + kept
        pieces.append(dot((decay * scores).astype(BF), g_h, TN))
        passed = dot((kept * scores).astype(BF), before)
        inner.append(jnp.sum(jnp.where(lower, passed, 0.0), axis=0, keepdims=True))
    steps = steps[0:HEADS] + jnp.concatenate(inner, axis=0)
    dq_ref[...] = -steps * jnp.exp(alog_ref[...])
    dx = jnp.concatenate(pieces, axis=1) + from_after + gf * skip_ref[...]
    dx_b = dx.astype(dx_ref.dtype)
    for q in range(dx_ref.shape[0]):
        dx_ref[q, 0, 0] = dx_b
    mixed_b = mixed.astype(BF)
    bc_ref[:, 0:NST] = (db + dot(mixed_b, c, TN)).astype(bc_ref.dtype)
    bc_ref[:, NST:] = (dc + dot(mixed_b, b)).astype(bc_ref.dtype)


def span_grads(me, x, g, b, c, parts, packs, alog, skip, half):
    cumr, cumc, sl, gl, dpre, dpost = parts
    spans = sl.shape[0] // 2
    base = half * spans
    once = lambda shape: pl.BlockSpec(shape, lambda i: (0,) * len(shape))
    lead = lambda shape: pl.BlockSpec((1, *shape), lambda i: (base + i, 0, 0))
    rows = lambda width: pl.BlockSpec((L, width), lambda i: (base + i, 0))
    return pl.pallas_call(
        grads_kernel,
        grid=(spans,),
        in_specs=[
            pl.BlockSpec(memory_space=pltpu.SMEM),
            rows(HP), rows(HP), rows(NST), rows(NST),
            lead((8, L)), lead((L, 8)), lead((HP, NST)), lead((HP, NST)),
            lead((8, NST)), lead((8, NST)),
            once(packs.shape), once(alog.shape), once(skip.shape),
        ],
        out_specs=[
            pl.BlockSpec((4, 1, 1, L, HP), lambda i: (0, i % 4, i // 4, 0, 0)),
            pl.BlockSpec((L, 2 * NST), lambda i: (i, 0)),
            pl.BlockSpec((HEADS, L), lambda i: (0, i)),
        ],
        out_shape=(
            jax.ShapeDtypeStruct((4, 4, spans // 4, L, HP), BF),
            jax.ShapeDtypeStruct((spans * L, 2 * NST), BF),
            jax.ShapeDtypeStruct((HEADS, spans * L), F32),
        ),
        scratch_shapes=[pltpu.VMEM((HP, NST), F32), pltpu.VMEM((HP, NST), F32)],
        cost_estimate=cost(10),
        name="span_grads",
    )(me, x, g, b, c, cumr, cumc, sl, gl, dpre, dpost, packs, alog, skip)


def routing_kernel(ids_ref, gates_ref, tgt_ref, out_ref):
    experts, slots = out_ref.shape
    tokens = ids_ref.shape[1]
    expert = lax.broadcasted_iota(jnp.int32, (experts, tokens), 0)
    slot = lax.broadcasted_iota(jnp.int32, (slots, tokens), 0)
    named = [(expert == ids_ref[k : k + 1, :]).astype(F32) for k in range(2)]
    earlier = (
        lax.broadcasted_iota(jnp.int32, (tokens, tokens), 0)
        < lax.broadcasted_iota(jnp.int32, (tokens, tokens), 1)
    ).astype(BF)
    counts = dot((named[0] + named[1]).astype(BF), earlier)
    tgt_ref[...] = jnp.zeros_like(tgt_ref)
    total = jnp.zeros((experts, slots), F32)
    for k in range(2):
        position = jnp.sum(named[k] * counts, axis=0, keepdims=True).astype(jnp.int32)
        tgt_ref[k : k + 1, :] = ids_ref[k : k + 1, :] * slots + position
        placed = (slot == position).astype(BF)
        total = total + dot((named[k] * gates_ref[k : k + 1, :]).astype(BF), placed, NT)
    out_ref[...] = total.astype(out_ref.dtype)


def routing(ids, gates):
    return pl.pallas_call(
        routing_kernel,
        out_shape=(
            jax.ShapeDtypeStruct((8, ids.shape[1]), jnp.int32),
            jax.ShapeDtypeStruct((16, 16), BF),
        ),
        cost_estimate=cost(2),
        name="routing",
    )(ids, gates)


def first_kernel(res_ref, tgt_ref, w_ref, out_ref):
    named = tgt_ref[...].astype(F32)
    named = jnp.concatenate([named, jnp.zeros_like(named)], axis=0).astype(BF)
    for q in range(4):
        for s in range(8):
            lanes = slice(128 * s, 128 * (s + 1))
            out_ref[q, 0:128, lanes] = res_ref[:, 512 * s + 128 * q : 512 * s + 128 * (q + 1)]
            out_ref[q, 128:144, lanes] = named
        for j in range(4):
            rows = slice(128 * q + 32 * j, 128 * q + 32 * (j + 1))
            out_ref[q, 144:176, 256 * j : 256 * (j + 1)] = w_ref[rows, :]


def first_exchange(residual, targets, weight):
    return pl.pallas_call(
        first_kernel,
        out_shape=jax.ShapeDtypeStruct((4, 176, 1024), BF),
        cost_estimate=cost(3),
        name="first_exchange",
    )(residual, targets, weight)


def rows_kernel(x_ref, w_ref, res_ref, out_ref, acc_ref):
    def step(e, carry):
        blocks = [w_ref[s, e % 4, e // 4] for s in range(2)]
        right = jnp.concatenate(
            [block[:, 256 * j : 256 * (j + 1)] for block in blocks for j in range(4)], axis=0
        )
        acc_ref[...] += dot(x_ref[e], right, NT)
        return carry

    acc_ref[...] = jnp.zeros_like(acc_ref)
    lax.fori_loop(0, 16, step, 0, unroll=16)
    slot = lax.broadcasted_iota(jnp.int32, (256, 128), 0).astype(F32)
    for k in range(2):
        total = acc_ref[128 * k : 128 * (k + 1), :]
        rows = (res_ref[k, 0:128, :].astype(F32) + total).astype(BF)
        named = res_ref[k, 128:144, 0:128].astype(F32)
        picks = (slot == named[0:1, :]) | (slot == named[1:2, :])
        out_ref[:, k] = dot(picks.astype(BF), rows).astype(BF).reshape(16, 16, 256)


def expert_rows(x, weight, residual, half):
    return pl.pallas_call(
        rows_kernel,
        grid=(4,),
        in_specs=[
            pl.BlockSpec((16, 256, 256), lambda s: (0, 0, 0)),
            pl.BlockSpec((2, 4, 4, 32, 1024), lambda s: (s, 0, 0, 0, 0)),
            pl.BlockSpec((2, 144, 256), lambda s: (half, 0, s)),
        ],
        out_specs=pl.BlockSpec((16, 2, 16, 256), lambda s: (0, 0, 0, s)),
        out_shape=jax.ShapeDtypeStruct((16, 2, 16, 1024), BF),
        scratch_shapes=[pltpu.VMEM((256, 256), F32)],
        compiler_params=pltpu.CompilerParams(vmem_limit_bytes=48 << 20),
        cost_estimate=cost(6),
        name="expert_rows",
    )(x, weight, residual)


def turned_kernel(w_ref, out_ref):
    for q in range(4):
        for s in range(8):
            out_ref[:, 1024 * q + 128 * s : 1024 * q + 128 * (s + 1)] = w_ref[
                :, 512 * s + 128 * q : 512 * s + 128 * (q + 1)
            ]


def turned(w):
    rows = 128
    spec = pl.BlockSpec((rows, w.shape[1]), lambda i: (i, 0))
    return pl.pallas_call(
        turned_kernel,
        grid=(w.shape[0] // rows,),
        in_specs=[spec],
        out_specs=spec,
        out_shape=jax.ShapeDtypeStruct(w.shape, w.dtype),
        cost_estimate=cost(6),
        name="turned",
    )(w)


def expert_kernel(half, at_ref, own, left, right, low, high, w_hbm, saved, gates, *rest):
    out, route_ref, xbuf, wbuf, sbuf, gbuf, obuf, up_ref, psum_ref, mixed_ref, grad_ref, sems, x_sems = (
        rest[-13:]
    )
    x_at, y_at = at_ref[0], at_ref[1]
    saved_copy = pltpu.make_async_copy(saved.at[y_at, :, half], sbuf.reshape(4, 128, 2, 896), sems.at[4])
    gates_copy = pltpu.make_async_copy(gates.at[y_at, :, half], gbuf.reshape(4, 128, 1), sems.at[5])
    lanes_of = lambda q: pl.ds(pl.multiple_of(q * 1024, 1024), 1024)
    weights_of = lambda q: pltpu.make_async_copy(
        w_hbm.at[:, lanes_of(q)], wbuf.at[:, lanes_of(q)], sems.at[q]
    )
    sources = [lax.rem(x_at + step, 4) for step in (0, 3, 1, 2)]
    for q in range(4):
        far = (low, q) if q < 2 else (high, q - 2)
        for j, (piece, at) in enumerate(((own, q), (left, q), (right, q), far)):
            for k in range(2):
                pltpu.make_async_copy(
                    piece.at[at, :, k], xbuf.at[q, sources[j], k], x_sems.at[q, j, k]
                ).start()
        weights_of(q).start()
    gates_copy.start()
    saved_copy.start()
    up_ref[...] = jnp.zeros_like(up_ref)

    def by_quarter(q, carry):
        for j in range(4):
            for k in range(2):
                pltpu.make_async_copy(
                    own.at[q, :, k], xbuf.at[q, sources[j], k], x_sems.at[q, j, k]
                ).wait()
        weights_of(q).wait()

        def tile(at, width):
            here = pl.ds(at, width)
            piece = xbuf[q].reshape(512, 1024)
            up_ref[:, here] += dot(piece, wbuf[here, lanes_of(q)], NT)

        def wide(i, carry):
            tile(pl.multiple_of(i * 256, 256), 256)
            return carry

        lax.fori_loop(0, 3, wide, 0)
        tile(768, 128)
        return carry

    lax.fori_loop(0, 4, by_quarter, 0)
    gates_copy.wait()
    saved_copy.wait()
    count = 32

    def group(j, carry):
        rows = pl.ds(pl.multiple_of(j * count, count), count)
        gate = gbuf[rows, :]
        routed = jnp.zeros((count, 128), F32)
        for n in range(7):
            lanes = slice(128 * n, 128 * (n + 1))
            mixed_ref[...] = sbuf[rows, :, lanes].reshape(2 * count, 128).astype(F32)
            gate_pre = mixed_ref[pl.ds(0, count, stride=2), :]
            up_pre = mixed_ref[pl.ds(1, count, stride=2), :]
            upstream = up_ref[rows, lanes]
            sigmoid = 1.0 / (1.0 + jnp.exp(-gate_pre))
            active = gate_pre * sigmoid
            weighted = gate * upstream
            routed = routed + active * up_pre * upstream
            grad_ref[pl.ds(0, count, stride=2), :] = (
                weighted * up_pre * sigmoid * (1.0 + gate_pre * (1.0 - sigmoid))
            )
            grad_ref[pl.ds(1, count, stride=2), :] = weighted * active
            obuf[rows, :, lanes] = grad_ref[...].astype(BF).reshape(count, 2, 128)
        psum_ref[rows, :] = routed
        return carry

    def out_of(j):
        rows = pl.ds(pl.multiple_of(j * 128, 128), 128)
        return pltpu.make_async_copy(obuf.at[rows], out.at[y_at, j, half], sems.at[6 + j])

    def block(j, carry):
        lax.fori_loop(j * (128 // count), (j + 1) * (128 // count), group, 0)
        out_of(j).start()
        return carry

    lax.fori_loop(0, 4, block, 0)
    ones = jnp.ones((8, 128), F32)
    route_ref[...] = dot(ones, psum_ref[...], NT, precision=lax.Precision.HIGHEST)
    for j in range(4):
        out_of(j).wait()


def expert_grads(half, at, pieces, weight, saved, gates, before):
    own, left, right, low, high = [p.reshape(-1, 4, 2, 16, 1024) for p in pieces]
    hbm = pl.BlockSpec(memory_space=pl.ANY)
    args = [at, own, left, right, low, high, weight, saved, gates]
    if before is not None:
        args.append(before)
    return pl.pallas_call(
        functools.partial(expert_kernel, half),
        in_specs=[pl.BlockSpec(memory_space=pltpu.SMEM)] + [hbm] * (len(args) - 1),
        out_specs=[hbm, pl.BlockSpec(memory_space=pltpu.VMEM)],
        out_shape=(
            jax.ShapeDtypeStruct(saved.shape, BF),
            jax.ShapeDtypeStruct((8, 512), F32),
        ),
        scratch_shapes=[
            pltpu.VMEM((4, 4, 2, 4, 16, 1024), BF),
            pltpu.VMEM((896, 4096), BF),
            pltpu.VMEM((512, 2, 896), BF),
            pltpu.VMEM((512, 1), F32),
            pltpu.VMEM((512, 2, 896), BF),
            pltpu.VMEM((512, 896), F32),
            pltpu.VMEM((512, 128), F32),
            pltpu.VMEM((64, 128), F32),
            pltpu.VMEM((64, 128), F32),
            pltpu.SemaphoreType.DMA((12,)),
            pltpu.SemaphoreType.DMA((4, 4, 2)),
        ],
        input_output_aliases={} if before is None else {9: 0},
        compiler_params=pltpu.CompilerParams(vmem_limit_bytes=56 << 20),
        cost_estimate=cost(12),
        name="expert_grads",
    )(*args)


SEQ = ("yl", "x")
QUAD = ("yh", "zh")
MEMB = ("zl", "core")
EXP = QUAD + MEMB
BOTH = SEQ + EXP


def a2a(array, axis):
    return lax.all_to_all(array, axis, split_axis=0, concat_axis=0, tiled=True)


def shifted(array, by):
    return lax.ppermute(array, "x", [(i, (i + by) % 4) for i in range(4)])


def other_row(array):
    return lax.ppermute(array, "yl", [(0, 1), (1, 0)])


def near_x(own):
    return (own, shifted(own, 1), shifted(own, -1))


def joined_x(pieces):
    own, left, right = pieces
    low = shifted(left[:8], 1)
    high = shifted(right[8:], -1)
    return (own, left, right, low, high)


def per_device(
    gates, expert_ids, saved_pre, w_down, residual_grad, in_weight,
    ssm_in, b_proj, c_proj, step_sizes, a_log, skip_gain, ssm_grad,
):
    targets, slot_gates = routing(expert_ids.T, gates.T)
    first = first_exchange(residual_grad, targets, in_weight)
    first = a2a(first, QUAD)
    weight = lax.all_gather(first[:, 144:176].reshape(128, 1024), SEQ + MEMB, axis=0, tiled=True)
    weight = weight.reshape(8, 4, 4, 32, 1024)

    alog = a_log.reshape(4, 1)
    skip = jnp.repeat(skip_gain, HDIM).reshape(1, HP)
    *parts, pack = local_states(ssm_in, ssm_grad, b_proj, c_proj, step_sizes, alog)
    first, pack = lax.optimization_barrier((first, pack))
    here = lax.axis_index(SEQ)
    later = lax.broadcasted_iota(jnp.int32, (8, HP, NST), 0) > here
    states = jnp.where(later, pack[:HP], pack[HP : 2 * HP])
    rest = jnp.concatenate([pack[2 * HP :], jnp.pad(slot_gates, ((0, 0), (0, 112)))], axis=0)
    packs = jnp.concatenate([states, jnp.broadcast_to(rest, (8, *rest.shape))], axis=1)
    packs = a2a(packs, SEQ)
    gate_rows = packs[:, HP + 16 :, 0:16].transpose(1, 0, 2)
    gate_rows = a2a(gate_rows.reshape(16, 128), EXP)
    down = turned(w_down[0])

    args = (here.reshape(1), ssm_in, ssm_grad, b_proj, c_proj, parts, packs, alog, skip)
    arrived, grads, moved = {}, {}, {}
    for half in (1, 0):
        x_part, bc_part, step_part = span_grads(*args, half)
        grads[half] = (bc_part, step_part)
        if half == 1:
            x_part, gate_rows = lax.optimization_barrier((x_part, gate_rows))
        moved[half] = a2a(x_part.reshape(16, 256, 256), EXP)
    rows = {}
    rows[1] = expert_rows(moved[1], weight, first, 1)
    rows[1], moved[0] = lax.optimization_barrier((rows[1], moved[0]))
    rows[0] = expert_rows(moved[0], weight, first, 0)
    for half in (1, 0):
        arrived[half] = a2a(rows[half].reshape(16, 32, 1024), EXP)

    gate_rows = gate_rows.reshape(16, 8, 16).transpose(1, 0, 2)
    gate_rows = gate_rows.astype(F32).reshape(2, 4, 2, 128, 1)
    near = near_x(arrived[1])
    across = other_row(arrived[1])
    mine = joined_x(near)
    cross_left = other_row(near[1])
    cross_right = other_row(near[2])
    theirs = joined_x((across, cross_left, cross_right))
    partner = other_row(arrived[0])
    local = near_x(arrived[0])
    local = joined_x(local)
    partner = near_x(partner)
    partner = joined_x(partner)
    sets = [(1, 0, mine), (0, 0, local), (0, 1, partner), (1, 1, theirs)]

    x_at, y_at = lax.axis_index("x"), lax.axis_index("yl")
    saved = saved_pre.reshape(2, 4, 2, 128, 2, 896)
    out, routes = None, {}
    for half, flip, pieces in sets:
        at = jnp.stack([x_at, y_at ^ flip]).astype(jnp.int32)
        out, route = expert_grads(half, at, pieces, down, saved, gate_rows, out)
        routes[half, flip] = route[0].reshape(4, 128)
    first, second = [
        jnp.stack([routes[0, flip], routes[1, flip]], axis=1).reshape(4, 256) for flip in (0, 1)
    ]
    low, high = [jnp.where(y_at == 0, a, b) for a, b in ((first, second), (second, first))]
    partial = jnp.concatenate([low, high], axis=0)
    both = jnp.concatenate([grads[0][0], grads[1][0]], axis=0).reshape(16, 128, 2 * NST)
    both = a2a(both, EXP)
    partial, both = lax.optimization_barrier((partial, both))
    totals = a2a(partial.reshape(128, 16), BOTH).reshape(8, 16, 16)
    totals = jnp.sum(totals, axis=0).reshape(256, 1)
    slot = lax.broadcasted_iota(jnp.int32, (256, 128), 0)
    route_grads = jnp.stack(
        [jnp.sum(jnp.where(slot == targets[k], totals, 0.0), axis=0) for k in range(2)], axis=1
    )

    both = jnp.sum(both.astype(F32), axis=0)
    step_grads = jnp.concatenate([grads[0][1], grads[1][1]], axis=1)
    pre_grads = out.reshape(1, 2048, 2, 896)
    return (pre_grads, route_grads, both[:, :NST], both[:, NST:], step_grads)


def solution(mesh):
    split = Mesh(mesh.devices.reshape(2, 4, 2, 2, 2, 2), BOTH)
    in_specs = (
        P(BOTH, None), P(BOTH, None), P(EXP, None, None, SEQ), P(EXP, SEQ, None), P(BOTH, None),
        P(SEQ, EXP), P(SEQ, EXP), P(SEQ, None), P(SEQ, None), P(EXP, SEQ), P(EXP), P(EXP),
        P(SEQ, EXP),
    )
    out_specs = (P(EXP, None, None, SEQ), P(BOTH, None), P(BOTH, None), P(BOTH, None), P(EXP, SEQ))

    return jax.shard_map(per_device, mesh=split, in_specs=in_specs, out_specs=out_specs, check_vma=False)
```
